64 devices in a mesh: dp: 4 (over x, y), tp: 16 (over z, core).
Axes of the slice: x: 2, y: 2, z: 8, core: 2. Of those that a mesh axis runs over, the one named last changes fastest.
The devices are a block of a 4x4x8 slice.
Arguments:
- hidden: bfloat16 [128, 3, 4096], P('dp'), parts along dimension 0
- draft_ids: int32 [128, 2], P('dp'), parts along dimension 0
- norm_gain: bfloat16 [4096], replicated
- head_w: bfloat16 [4096, 32000], P(None, 'tp')
Outputs:
- output 1: float32 [128, 2], P('dp'), parts along dimension 0
- output 2: float32 [128, 3], P('dp'), parts along dimension 0
- output 3: float32 [128, 3], P('dp'), parts along dimension 0
There are 4 independent parts. The reference program is written for one: setup_inputs(seed, part) draws one part's arguments, and reference() takes and returns one part's arrays. A program takes and returns all parts, laid end to end along the dimension named above; an argument that names none is the same for every part.
All inputs are finite; a program needn't handle non-finite values.
Results may differ from the reference program's by a relative error of at most 0.001.
Values sent between devices are 32-bit elements.
A program may use at most 768 MiB of HBM per device.

```python
import jax
import jax.numpy as jnp
from jax import lax

DIM = 4096
VOCAB = 32000
BATCH = 32
DRAFTS = 2
NORM_EPS = 1e-5


def setup_inputs(seed: int = 0, part: int = 0) -> dict:
    root_key = jax.random.key(seed)
    shared_key, part_base = jax.random.split(root_key)
    part_key = jax.random.fold_in(part_base, part)
    key_x, key_d = jax.random.split(part_key)
    key_g, key_w, key_hot = jax.random.split(shared_key, 3)
    hidden = jax.random.normal(key_x, (BATCH, DRAFTS + 1, DIM), jnp.float32)
    draft_ids = jax.random.randint(key_d, (BATCH, DRAFTS), 0, VOCAB, jnp.int32)
    norm_gain = 1.0 + 0.2 * jax.random.normal(key_g, (DIM,), jnp.float32)
    hot_cols = jax.random.randint(key_hot, (VOCAB,), 0, 64, jnp.int32) == 0
    col_scale = jnp.where(hot_cols, 3.5, 2.0) * DIM ** -0.5
    head_w = jax.random.normal(key_w, (DIM, VOCAB), jnp.float32) * col_scale
    return {'hidden': hidden.astype(jnp.bfloat16), 'draft_ids': draft_ids, 'norm_gain': norm_gain.astype(jnp.bfloat16), 'head_w': head_w.astype(jnp.bfloat16)}


def rms_norm(hidden, norm_gain):
    wide_x = hidden.astype(jnp.float32)
    inv_rms = lax.rsqrt(jnp.mean(wide_x * wide_x, axis=-1, keepdims=True) + NORM_EPS)
    return (wide_x * inv_rms * norm_gain.astype(jnp.float32)).astype(jnp.bfloat16)


def reference(hidden, draft_ids, norm_gain, head_w):
    def one_sequence(seq_pair):
        seq_rows, seq_ids = seq_pair
        normed = rms_norm(seq_rows, norm_gain)
        logits = jnp.dot(normed, head_w, preferred_element_type=jnp.float32)
        row_max = jnp.max(logits, axis=-1)
        shifted = logits - row_max[:, None]
        exp_vals = jnp.exp(shifted)
        exp_sum = jnp.sum(exp_vals, axis=-1)
        weighted = jnp.sum(exp_vals * shifted, axis=-1)
        log_sum = jnp.log(exp_sum)
        log_norm = row_max + log_sum
        entropy = log_sum - weighted / exp_sum
        drafts = seq_ids.shape[0]
        picked = jnp.take_along_axis(logits[:drafts], seq_ids[:, None], axis=1)[:, 0]
        return picked - log_norm[:drafts], log_norm, entropy
    draft_logp, log_norm, entropy = lax.map(one_sequence, (hidden, draft_ids))
    return draft_logp, log_norm, entropy
```

```python
import functools

import jax
import jax.numpy as jnp
from jax import lax
from jax.experimental import pallas as pl
from jax.experimental.pallas import tpu as pltpu
from jax.sharding import PartitionSpec as P

NORM_EPS = 1e-5
LANES = 128
SUBLANES = 8


def chunk_bounds(total):
    step = 256
    return [(start, min(step, total - start)) for start in range(0, total, step)]


def head_kernel(
    peers,
    x_hbm, ids_ref, gain_ref, w_hbm,
    logp_ref, norm_ref, ent_ref,
    x_vmem, n_vmem, w_vmem, own, recv,
    x_sem, w_sem, send_sem, recv_sem,
):
    steps, seqs, dim = x_vmem.shape
    rows = steps * seqs
    drafts = ids_ref.shape[0]
    cols = w_vmem.shape[0]
    chunks = chunk_bounds(cols)
    me = lax.axis_index('tp')

    x_copies = [pltpu.make_async_copy(x_hbm.at[t], x_vmem.at[t], x_sem.at[t]) for t in range(steps)]
    w_copies = [
        pltpu.make_async_copy(w_hbm.at[pl.ds(start, size)], w_vmem.at[pl.ds(start, size)], w_sem.at[i])
        for i, (start, size) in enumerate(chunks)
    ]
    for copy in x_copies + w_copies:
        copy.start()

    barrier = pltpu.get_barrier_semaphore()
    for hop in range(1, peers):
        pl.semaphore_signal(
            barrier, inc=1, device_id={'tp': lax.rem(me + hop, peers)}, device_id_type=pl.DeviceIdType.MESH
        )

    ids = jnp.concatenate(
        [ids_ref[pl.ds(t, 1), :] for t in range(drafts)] + [jnp.full((1, rows - drafts * seqs), -1, jnp.int32)], axis=1
    )
    local_ids = ids - me * cols

    gain = gain_ref[...].astype(jnp.float32)
    for t in range(steps):
        x_copies[t].wait()
        wide_x = x_vmem[t].astype(jnp.float32)
        inv_rms = lax.rsqrt(jnp.mean(wide_x * wide_x, axis=-1, keepdims=True) + NORM_EPS)
        n_vmem[pl.ds(t * seqs, seqs), :] = (wide_x * inv_rms * gain).astype(jnp.bfloat16)

    groups = (SUBLANES, rows)
    top = exp_sum = weighted = picked = None
    for i, (start, size) in enumerate(chunks):
        w_copies[i].wait()
        logits = lax.dot_general(
            w_vmem[pl.ds(start, size), :], n_vmem[...], (((1,), (1,)), ((), ())),
            preferred_element_type=jnp.float32,
        )
        tiles = logits.reshape(size // SUBLANES, SUBLANES, rows)
        col_ids = lax.broadcasted_iota(jnp.int32, tiles.shape, 0) * SUBLANES + (
            lax.broadcasted_iota(jnp.int32, tiles.shape, 1) + start
        )
        hit = jnp.sum(jnp.where(col_ids == local_ids[None], tiles, 0.0), axis=0)
        chunk_top = jnp.max(tiles, axis=0)
        new_top = chunk_top if top is None else jnp.maximum(top, chunk_top)
        shifted = tiles - new_top[None]
        exp_vals = jnp.exp(shifted)
        chunk_sum = jnp.sum(exp_vals, axis=0)
        chunk_weighted = jnp.sum(exp_vals * shifted, axis=0)
        if top is None:
            exp_sum, weighted, picked = chunk_sum, chunk_weighted, hit
        else:
            drop = top - new_top
            scale = jnp.exp(drop)
            weighted = chunk_weighted + scale * (weighted + exp_sum * drop)
            exp_sum = chunk_sum + scale * exp_sum
            picked = picked + hit
        top = new_top

    all_top = jnp.max(top, axis=0, keepdims=True)
    drop = top - all_top
    scale = jnp.exp(drop)
    own_sum = jnp.sum(scale * exp_sum, axis=0, keepdims=True)
    own_weighted = jnp.sum(scale * (weighted + exp_sum * drop), axis=0, keepdims=True)
    own_picked = jnp.sum(picked, axis=0, keepdims=True)
    stats = jnp.concatenate([all_top, own_sum, own_weighted, own_picked], axis=0)
    stats = jnp.concatenate([stats, jnp.zeros((stats.shape[0], LANES - rows), jnp.float32)], axis=1)
    own[...] = stats
    recv[me] = stats

    pl.semaphore_wait(barrier, peers - 1)
    for hop in range(1, peers):
        pltpu.make_async_remote_copy(
            src_ref=own, dst_ref=recv.at[me], send_sem=send_sem, recv_sem=recv_sem,
            device_id={'tp': lax.rem(me + hop, peers)}, device_id_type=pl.DeviceIdType.MESH,
        ).start()
    others = recv.at[pl.ds(0, peers - 1)]
    pltpu.make_async_copy(others, others, recv_sem).wait()

    parts = recv[...]
    tops = parts[:, 0:1, :rows]
    full_top = jnp.max(tops, axis=0)
    drop = tops - full_top[None]
    scale = jnp.exp(drop)
    sums = parts[:, 1:2, :rows]
    full_sum = jnp.sum(scale * sums, axis=0)
    full_weighted = jnp.sum(scale * (parts[:, 2:3, :rows] + sums * drop), axis=0)
    full_picked = jnp.sum(parts[:, 3:4, :rows], axis=0)
    log_sum = jnp.log(full_sum)
    log_norm = full_top + log_sum
    entropy = log_sum - full_weighted / full_sum
    logp = full_picked - log_norm
    for t in range(steps):
        lanes = slice(t * seqs, (t + 1) * seqs)
        norm_ref[pl.ds(t, 1), :] = log_norm[:, lanes]
        ent_ref[pl.ds(t, 1), :] = entropy[:, lanes]
        if t < drafts:
            logp_ref[pl.ds(t, 1), :] = logp[:, lanes]
    pltpu.make_async_copy(others, others, send_sem).wait()


def solution(mesh):
    peers = mesh.shape['tp']

    def per_device(hidden, draft_ids, norm_gain, head_w):
        seqs, steps, dim = hidden.shape
        drafts = draft_ids.shape[1]
        cols = head_w.shape[1]
        rows = steps * seqs
        chunks = chunk_bounds(cols)
        vmem = pl.BlockSpec(memory_space=pltpu.VMEM)
        anywhere = pl.BlockSpec(memory_space=pl.ANY)
        logp, log_norm, entropy = pl.pallas_call(
            functools.partial(head_kernel, peers),
            out_shape=(
                jax.ShapeDtypeStruct((drafts, seqs), jnp.float32),
                jax.ShapeDtypeStruct((steps, seqs), jnp.float32),
                jax.ShapeDtypeStruct((steps, seqs), jnp.float32),
            ),
            in_specs=[anywhere, vmem, vmem, anywhere],
            out_specs=(vmem, vmem, vmem),
            scratch_shapes=[
                pltpu.VMEM((steps, seqs, dim), jnp.bfloat16),
                pltpu.VMEM((rows, dim), jnp.bfloat16),
                pltpu.VMEM((cols, dim), jnp.bfloat16),
                pltpu.VMEM((4, LANES), jnp.float32),
                pltpu.VMEM((peers, 4, LANES), jnp.float32),
                pltpu.SemaphoreType.DMA((steps,)),
                pltpu.SemaphoreType.DMA((len(chunks),)),
                pltpu.SemaphoreType.DMA,
                pltpu.SemaphoreType.DMA,
            ],
            compiler_params=pltpu.CompilerParams(
                collective_id=0, has_side_effects=True, vmem_limit_bytes=60 * 1024 * 1024
            ),
        )(hidden.transpose(1, 0, 2), draft_ids.T, norm_gain.reshape(1, dim), head_w.T)
        return logp.T, log_norm.T, entropy.T

    specs_in = (P('dp', None, None), P('dp', None), P(None), P(None, 'tp'))
    specs_out = (P('dp', None), P('dp', None), P('dp', None))
    return jax.shard_map(per_device, mesh=mesh, in_specs=specs_in, out_specs=specs_out, check_vma=False)
```

```python
import functools

import jax
import jax.numpy as jnp
from jax import lax
from jax.experimental import pallas as pl
from jax.experimental.pallas import tpu as pltpu
from jax.sharding import PartitionSpec as P

NORM_EPS = 1e-5
LANES = 128
SUBLANES = 8
TILE = 256
STEP_ROWS = 400


def chunk_bounds(total):
    return [(start, min(STEP_ROWS, total - start)) for start in range(0, total, STEP_ROWS)]


def head_kernel(
    peers,
    x_hbm, ids_hbm, gain_hbm, w_hbm,
    logp_ref, norm_ref, ent_ref,
    x_vmem, ids_vmem, gain_vmem, n_vmem, w_vmem, z_vmem, own, recv,
    x_sem, small_sem, w_sem, send_sem, recv_sem,
):
    steps, seqs, dim = x_vmem.shape
    rows = steps * seqs
    drafts = ids_vmem.shape[0]
    cols = w_vmem.shape[0]
    chunks = chunk_bounds(cols)
    me = lax.axis_index('tp')

    ids_copy = pltpu.make_async_copy(ids_hbm, ids_vmem, small_sem.at[0])
    gain_copy = pltpu.make_async_copy(gain_hbm, gain_vmem, small_sem.at[1])
    x_copies = [pltpu.make_async_copy(x_hbm.at[t], x_vmem.at[t], x_sem.at[t]) for t in range(steps)]
    w_copies = [
        pltpu.make_async_copy(w_hbm.at[pl.ds(start, size)], w_vmem.at[pl.ds(start, size)], w_sem.at[i])
        for i, (start, size) in enumerate(chunks)
    ]
    for copy in x_copies + [gain_copy, ids_copy]:
        copy.start()
    for copy in w_copies:
        copy.start()

    barrier = pltpu.get_barrier_semaphore()
    for hop in range(1, peers):
        pl.semaphore_signal(
            barrier, inc=1, device_id={'tp': lax.rem(me + hop, peers)}, device_id_type=pl.DeviceIdType.MESH
        )

    for t in range(steps):
        x_copies[t].wait()
        if t == 0:
            gain_copy.wait()
        wide = [x_vmem[t, :, pl.ds(c, LANES)].astype(jnp.float32) for c in range(0, dim, LANES)]
        squares = [x * x for x in wide]
        while len(squares) > 1:
            squares = [a + b for a, b in zip(squares[::2], squares[1::2])]
        mean = jnp.sum(squares[0], axis=-1, keepdims=True) / dim
        inv_rms = lax.rsqrt(mean + NORM_EPS)
        for c, x in enumerate(wide):
            gain = gain_vmem[pl.ds(c, 1), :].astype(jnp.float32)
            n_vmem[pl.ds(t * seqs, seqs), pl.ds(c * LANES, LANES)] = (x * inv_rms * gain).astype(jnp.bfloat16)

    ids_copy.wait()
    ids = jnp.concatenate(
        [ids_vmem[pl.ds(t, 1), :] for t in range(drafts)] + [jnp.full((1, rows - drafts * seqs), -1, jnp.int32)],
        axis=1,
    )
    local_ids = ids - me * cols

    def stats_of(carry, start, size, tiles):
        top, exp_sum, weighted, picked = carry
        tiles = tiles.reshape(size // SUBLANES, SUBLANES, rows)
        col_ids = lax.broadcasted_iota(jnp.int32, tiles.shape, 0) * SUBLANES + (
            lax.broadcasted_iota(jnp.int32, tiles.shape, 1) + start
        )
        hit = jnp.sum(jnp.where(col_ids == local_ids[None], tiles, 0.0), axis=0)
        chunk_top = jnp.max(tiles, axis=0)
        new_top = chunk_top if top is None else jnp.maximum(top, chunk_top)
        shifted = tiles - new_top[None]
        exp_vals = jnp.exp(shifted)
        chunk_sum = jnp.sum(exp_vals, axis=0)
        chunk_weighted = jnp.sum(exp_vals * shifted, axis=0)
        if top is None:
            return new_top, chunk_sum, chunk_weighted, hit
        drop = top - new_top
        scale = jnp.exp(drop)
        return (
            new_top,
            chunk_sum + scale * exp_sum,
            chunk_weighted + scale * (weighted + exp_sum * drop),
            picked + hit,
        )

    halves = 2
    per_half = dim // TILE // halves

    def run(accs):
        carry = (None,) * 4

        def drain(i, carry):
            start, size = chunks[i]
            low, high = (pltpu.matmul_pop(acc)[:, :LANES] for acc in accs[i % 2])
            return stats_of(carry, start, size, low + high)

        pending = None
        for i, (start, size) in enumerate(chunks):
            w_copies[i].wait()
            outs = []
            part = size // 2
            for half in range(2):
                outs.append(lax.dot_general(w_vmem[pl.ds(start + half * part, part), :], n_vmem[...], (((1,), (1,)), ((), ())), preferred_element_type=jnp.float32))
            if pending is not None:
                carry = stats_of(carry, *pending)
            pending = (start, size, jnp.concatenate(outs, axis=0))
        return stats_of(carry, *pending)

    def body(*refs):
        top, exp_sum, weighted, picked = run(None)

        all_top = jnp.max(top, axis=0, keepdims=True)
        drop = top - all_top
        scale = jnp.exp(drop)
        own_sum = jnp.sum(scale * exp_sum, axis=0, keepdims=True)
        own_weighted = jnp.sum(scale * (weighted + exp_sum * drop), axis=0, keepdims=True)
        own_picked = jnp.sum(picked, axis=0, keepdims=True)
        stats = jnp.concatenate([all_top, own_sum, own_weighted, own_picked], axis=0)
        stats = jnp.concatenate([stats, jnp.zeros((4, LANES - rows), jnp.float32)], axis=1)
        own[...] = stats
        recv[me] = stats

    body()

    pl.semaphore_wait(barrier, peers - 1)
    for hop in range(1, peers):
        pltpu.make_async_remote_copy(
            src_ref=own, dst_ref=recv.at[me], send_sem=send_sem, recv_sem=recv_sem,
            device_id={'tp': lax.rem(me + hop, peers)}, device_id_type=pl.DeviceIdType.MESH,
        ).start()
    others = recv.at[pl.ds(0, peers - 1)]
    pltpu.make_async_copy(others, others, recv_sem).wait()

    parts = recv[...]
    tops = parts[:, 0:1, :rows]
    full_top = jnp.max(tops, axis=0)
    drop = tops - full_top[None]
    scale = jnp.exp(drop)
    sums = parts[:, 1:2, :rows]
    full_sum = jnp.sum(scale * sums, axis=0)
    full_weighted = jnp.sum(scale * (parts[:, 2:3, :rows] + sums * drop), axis=0)
    full_picked = jnp.sum(parts[:, 3:4, :rows], axis=0)
    log_sum = jnp.log(full_sum)
    log_norm = full_top + log_sum
    entropy = log_sum - full_weighted / full_sum
    logp = full_picked - log_norm
    for t in range(steps):
        lanes = slice(t * seqs, (t + 1) * seqs)
        norm_ref[pl.ds(t, 1), :] = log_norm[:, lanes]
        ent_ref[pl.ds(t, 1), :] = entropy[:, lanes]
        if t < drafts:
            logp_ref[pl.ds(t, 1), :] = logp[:, lanes]
    pltpu.make_async_copy(others, others, send_sem).wait()


def solution(mesh):
    peers = mesh.shape['tp']

    def per_device(hidden, draft_ids, norm_gain, head_w):
        seqs, steps, dim = hidden.shape
        drafts = draft_ids.shape[1]
        cols = head_w.shape[1]
        rows = steps * seqs
        chunks = chunk_bounds(cols)
        vmem = pl.BlockSpec(memory_space=pltpu.VMEM)
        anywhere = pl.BlockSpec(memory_space=pl.ANY)
        logp, log_norm, entropy = pl.pallas_call(
            functools.partial(head_kernel, peers),
            out_shape=(
                jax.ShapeDtypeStruct((drafts, seqs), jnp.float32),
                jax.ShapeDtypeStruct((steps, seqs), jnp.float32),
                jax.ShapeDtypeStruct((steps, seqs), jnp.float32),
            ),
            in_specs=[anywhere] * 4,
            out_specs=(vmem, vmem, vmem),
            scratch_shapes=[
                pltpu.VMEM((steps, seqs, dim), jnp.bfloat16),
                pltpu.VMEM((drafts, seqs), jnp.int32),
                pltpu.VMEM((dim // LANES, LANES), jnp.bfloat16),
                pltpu.VMEM((rows, dim), jnp.bfloat16),
                pltpu.VMEM((cols, dim), jnp.bfloat16),
                pltpu.VMEM((STEP_ROWS, LANES), jnp.float32),
                pltpu.VMEM((4, LANES), jnp.float32),
                pltpu.VMEM((peers, 4, LANES), jnp.float32),
                pltpu.SemaphoreType.DMA((steps,)),
                pltpu.SemaphoreType.DMA((2,)),
                pltpu.SemaphoreType.DMA((len(chunks),)),
                pltpu.SemaphoreType.DMA,
                pltpu.SemaphoreType.DMA,
            ],
            compiler_params=pltpu.CompilerParams(
                collective_id=0, has_side_effects=True, vmem_limit_bytes=60 * 1024 * 1024
            ),
        )(hidden.transpose(1, 0, 2), draft_ids.T, norm_gain.reshape(dim // LANES, LANES), head_w.T)
        return logp.T, log_norm.T, entropy.T

    specs_in = (P('dp', None, None), P('dp', None), P(None), P(None, 'tp'))
    specs_out = (P('dp', None), P('dp', None), P('dp', None))
    return jax.shard_map(per_device, mesh=mesh, in_specs=specs_in, out_specs=specs_out, check_vma=False)
```

```python
import functools

import jax
import jax.numpy as jnp
from jax import lax
from jax.experimental import pallas as pl
from jax.experimental.pallas import tpu as pltpu
from jax.sharding import PartitionSpec as P

NORM_EPS = 1e-5
LANES = 128
SUBLANES = 8
TILE = 256
STEP_ROWS = 400


def chunk_bounds(total):
    return [(start, min(STEP_ROWS, total - start)) for start in range(0, total, STEP_ROWS)]


def head_kernel(
    peers,
    x_hbm, ids_hbm, gain_hbm, w_hbm,
    logp_ref, norm_ref, ent_ref,
    x_vmem, ids_vmem, gain_vmem, n_vmem, w_vmem, z_vmem, own, recv,
    x_sem, small_sem, w_sem, send_sem, recv_sem,
):
    steps, seqs, dim = x_vmem.shape
    rows = steps * seqs
    drafts = ids_vmem.shape[0]
    cols = w_vmem.shape[0]
    chunks = chunk_bounds(cols)
    me = lax.axis_index('tp')

    ids_copy = pltpu.make_async_copy(ids_hbm, ids_vmem, small_sem.at[0])
    gain_copy = pltpu.make_async_copy(gain_hbm, gain_vmem, small_sem.at[1])
    x_copies = [pltpu.make_async_copy(x_hbm.at[t], x_vmem.at[t], x_sem.at[t]) for t in range(steps)]
    w_copies = [
        pltpu.make_async_copy(w_hbm.at[pl.ds(start, size)], w_vmem.at[pl.ds(start, size)], w_sem.at[i])
        for i, (start, size) in enumerate(chunks)
    ]
    for copy in x_copies + [gain_copy, ids_copy]:
        copy.start()
    for copy in w_copies:
        copy.start()

    barrier = pltpu.get_barrier_semaphore()
    for hop in range(1, peers):
        pl.semaphore_signal(
            barrier, inc=1, device_id={'tp': lax.rem(me + hop, peers)}, device_id_type=pl.DeviceIdType.MESH
        )

    for t in range(steps):
        x_copies[t].wait()
        if t == 0:
            gain_copy.wait()
        wide = [x_vmem[t, :, pl.ds(c, LANES)].astype(jnp.float32) for c in range(0, dim, LANES)]
        squares = [x * x for x in wide]
        while len(squares) > 1:
            squares = [a + b for a, b in zip(squares[::2], squares[1::2])]
        mean = jnp.sum(squares[0], axis=-1, keepdims=True) / dim
        inv_rms = lax.rsqrt(mean + NORM_EPS)
        for c, x in enumerate(wide):
            gain = gain_vmem[pl.ds(c, 1), :].astype(jnp.float32)
            n_vmem[pl.ds(t * seqs, seqs), pl.ds(c * LANES, LANES)] = (x * inv_rms * gain).astype(jnp.bfloat16)

    ids_copy.wait()
    ids = jnp.concatenate(
        [ids_vmem[pl.ds(t, 1), :] for t in range(drafts)] + [jnp.full((1, rows - drafts * seqs), -1, jnp.int32)],
        axis=1,
    )
    local_ids = ids - me * cols

    def stats_of(carry, start, size, tiles):
        top, exp_sum, weighted, picked = carry
        tiles = tiles.reshape(size // SUBLANES, SUBLANES, rows)
        col_ids = lax.broadcasted_iota(jnp.int32, tiles.shape, 0) * SUBLANES + (
            lax.broadcasted_iota(jnp.int32, tiles.shape, 1) + start
        )
        hit = jnp.sum(jnp.where(col_ids == local_ids[None], tiles, 0.0), axis=0)
        chunk_top = jnp.max(tiles, axis=0)
        new_top = chunk_top if top is None else jnp.maximum(top, chunk_top)
        shifted = tiles - new_top[None]
        exp_vals = jnp.exp(shifted)
        chunk_sum = jnp.sum(exp_vals, axis=0)
        chunk_weighted = jnp.sum(exp_vals * shifted, axis=0)
        if top is None:
            return new_top, chunk_sum, chunk_weighted, hit
        drop = top - new_top
        scale = jnp.exp(drop)
        return (
            new_top,
            chunk_sum + scale * exp_sum,
            chunk_weighted + scale * (weighted + exp_sum * drop),
            picked + hit,
        )

    halves = 2
    per_half = dim // TILE // halves

    def run(accs):
        carry = (None,) * 4

        def drain(i, carry):
            start, size = chunks[i]
            low, high = (pltpu.matmul_pop(acc)[:, :LANES] for acc in accs[i % 2])
            return stats_of(carry, start, size, low + high)

        pending = None
        for i, (start, size) in enumerate(chunks):
            w_copies[i].wait()
            outs = []
            part = size // 2
            for half in range(2):
                outs.append(lax.dot_general(w_vmem[pl.ds(start + half * part, part), :], n_vmem[...], (((1,), (1,)), ((), ())), preferred_element_type=jnp.float32))
            if pending is not None:
                carry = stats_of(carry, *pending)
            pending = (start, size, jnp.concatenate(outs, axis=0))
        return stats_of(carry, *pending)

    def body(*refs):
        top, exp_sum, weighted, picked = run(None)

        all_top = jnp.max(top, axis=0, keepdims=True)
        drop = top - all_top
        scale = jnp.exp(drop)
        own_sum = jnp.sum(scale * exp_sum, axis=0, keepdims=True)
        own_weighted = jnp.sum(scale * (weighted + exp_sum * drop), axis=0, keepdims=True)
        own_picked = jnp.sum(picked, axis=0, keepdims=True)
        stats = jnp.concatenate([all_top, own_sum, own_weighted, own_picked], axis=0)
        stats = jnp.concatenate([stats, jnp.zeros((4, LANES - rows), jnp.float32)], axis=1)
        own[...] = stats
        recv[me] = stats

    body()

    pl.semaphore_wait(barrier, peers - 1)
    for hop in range(1, peers):
        pltpu.make_async_remote_copy(
            src_ref=own, dst_ref=recv.at[me], send_sem=send_sem, recv_sem=recv_sem,
            device_id={'tp': lax.rem(me + hop, peers)}, device_id_type=pl.DeviceIdType.MESH,
        ).start()
    others = recv.at[pl.ds(0, peers - 1)]
    pltpu.make_async_copy(others, others, recv_sem).wait()

    parts = recv[...]
    tops = parts[:, 0:1, :rows]
    full_top = jnp.max(tops, axis=0)
    drop = tops - full_top[None]
    scale = jnp.exp(drop)
    sums = parts[:, 1:2, :rows]
    full_sum = jnp.sum(scale * sums, axis=0)
    full_weighted = jnp.sum(scale * (parts[:, 2:3, :rows] + sums * drop), axis=0)
    full_picked = jnp.sum(parts[:, 3:4, :rows], axis=0)
    log_sum = jnp.log(full_sum)
    log_norm = full_top + log_sum
    entropy = log_sum - full_weighted / full_sum
    logp = full_picked - log_norm
    for t in range(steps):
        lanes = slice(t * seqs, (t + 1) * seqs)
        norm_ref[pl.ds(t, 1), :] = log_norm[:, lanes]
        ent_ref[pl.ds(t, 1), :] = entropy[:, lanes]
        if t < drafts:
            logp_ref[pl.ds(t, 1), :] = logp[:, lanes]
    pltpu.make_async_copy(others, others, send_sem).wait()


def store_kernel(*refs):
    count = (len(refs) - 1) // 2
    copies = [pltpu.make_async_copy(refs[i], refs[count + i], refs[-1].at[i]) for i in range(count)]
    for copy in copies:
        copy.start()
    for copy in copies:
        copy.wait()


def solution(mesh):
    peers = mesh.shape['tp']

    def per_device(hidden, draft_ids, norm_gain, head_w):
        seqs, steps, dim = hidden.shape
        drafts = draft_ids.shape[1]
        cols = head_w.shape[1]
        rows = steps * seqs
        chunks = chunk_bounds(cols)
        vmem = pl.BlockSpec(memory_space=pltpu.VMEM)
        anywhere = pl.BlockSpec(memory_space=pl.ANY)
        results = pl.pallas_call(
            functools.partial(head_kernel, peers),
            out_shape=(
                pltpu.VMEM((drafts, seqs), jnp.float32),
                pltpu.VMEM((steps, seqs), jnp.float32),
                pltpu.VMEM((steps, seqs), jnp.float32),
            ),
            in_specs=[anywhere] * 4,
            out_specs=(vmem, vmem, vmem),
            scratch_shapes=[
                pltpu.VMEM((steps, seqs, dim), jnp.bfloat16),
                pltpu.VMEM((drafts, seqs), jnp.int32),
                pltpu.VMEM((dim // LANES, LANES), jnp.bfloat16),
                pltpu.VMEM((rows, dim), jnp.bfloat16),
                pltpu.VMEM((cols, dim), jnp.bfloat16),
                pltpu.VMEM((STEP_ROWS, LANES), jnp.float32),
                pltpu.VMEM((4, LANES), jnp.float32),
                pltpu.VMEM((peers, 4, LANES), jnp.float32),
                pltpu.SemaphoreType.DMA((steps,)),
                pltpu.SemaphoreType.DMA((2,)),
                pltpu.SemaphoreType.DMA((len(chunks),)),
                pltpu.SemaphoreType.DMA,
                pltpu.SemaphoreType.DMA,
            ],
            compiler_params=pltpu.CompilerParams(
                collective_id=0, has_side_effects=True, vmem_limit_bytes=60 * 1024 * 1024
            ),
        )(hidden.transpose(1, 0, 2), draft_ids.T, norm_gain.reshape(dim // LANES, LANES), head_w.T)
        logp, log_norm, entropy = pl.pallas_call(
            store_kernel,
            out_shape=tuple(jax.ShapeDtypeStruct(r.shape, r.dtype) for r in results),
            in_specs=[vmem] * len(results),
            out_specs=(anywhere,) * len(results),
            scratch_shapes=[pltpu.SemaphoreType.DMA((len(results),))],
        )(*(pltpu.with_memory_space_constraint(r, pltpu.VMEM) for r in results))
        return logp.T, log_norm.T, entropy.T

    specs_in = (P('dp', None, None), P('dp', None), P(None), P(None, 'tp'))
    specs_out = (P('dp', None), P('dp', None), P('dp', None))
    return jax.shard_map(per_device, mesh=mesh, in_specs=specs_in, out_specs=specs_out, check_vma=False)
```

```python
import functools

import jax
import jax.numpy as jnp
from jax import lax
from jax.experimental import pallas as pl
from jax.experimental.pallas import tpu as pltpu
from jax.sharding import PartitionSpec as P

NORM_EPS = 1e-5
LANES = 128
SUBLANES = 8
PACKED = 16
CFG = {'sizes': (400,) * 5, 'window': 2}


def bounds_of(total, sizes):
    out, start = [], 0
    for size in sizes:
        size = min(size, total - start)
        if size:
            out.append((start, size))
        start += size
    out.extend((begin, min(sizes[-1], total - begin)) for begin in range(start, total, sizes[-1]))
    return out


def stats_of(carry, local_ids, start, tiles):
    top, exp_sum, weighted, picked = carry
    size, lanes = tiles.shape
    tiles = tiles.reshape(size // SUBLANES, SUBLANES, lanes)
    col_ids = lax.broadcasted_iota(jnp.int32, tiles.shape, 0) * SUBLANES + (
        lax.broadcasted_iota(jnp.int32, tiles.shape, 1) + start
    )
    hit = jnp.sum(jnp.where(col_ids == local_ids[None, :, :lanes], tiles, 0.0), axis=0)
    chunk_top = jnp.max(tiles, axis=0)
    new_top = chunk_top if top is None else jnp.maximum(top, chunk_top)
    shifted = tiles - new_top[None]
    exp_vals = jnp.exp(shifted)
    chunk_sum = jnp.sum(exp_vals, axis=0)
    chunk_weighted = jnp.sum(exp_vals * shifted, axis=0)
    if top is None:
        return new_top, chunk_sum, chunk_weighted, hit
    drop = top - new_top
    scale = jnp.exp(drop)
    return (
        new_top,
        chunk_sum + scale * exp_sum,
        chunk_weighted + scale * (weighted + exp_sum * drop),
        picked + hit,
    )


def fold(carry):
    top, exp_sum, weighted, picked = carry
    all_top = jnp.max(top, axis=0, keepdims=True)
    drop = top - all_top
    scale = jnp.exp(drop)
    rows = [
        all_top,
        jnp.sum(scale * exp_sum, axis=0, keepdims=True),
        jnp.sum(scale * (weighted + exp_sum * drop), axis=0, keepdims=True),
        jnp.sum(picked, axis=0, keepdims=True),
    ]
    stats = jnp.concatenate(rows, axis=0)
    lanes = stats.shape[1]
    if lanes < LANES:
        stats = jnp.concatenate([stats, jnp.zeros((stats.shape[0], LANES - lanes), jnp.float32)], axis=1)
    return stats


def local_scratch(steps, seqs, drafts, dim, cols, pieces):
    return [
        pltpu.VMEM((steps, seqs, dim), jnp.bfloat16),
        pltpu.VMEM((drafts, seqs), jnp.int32),
        pltpu.VMEM((dim // LANES, LANES), jnp.bfloat16),
        pltpu.VMEM((dim // LANES, LANES), jnp.float32),
        pltpu.VMEM((steps * seqs, dim), jnp.bfloat16),
        pltpu.VMEM((cols, dim), jnp.bfloat16),
        pltpu.SemaphoreType.DMA((steps,)),
        pltpu.SemaphoreType.DMA((2,)),
        pltpu.SemaphoreType.DMA((pieces,)),
    ]


def local_stats(cfg, me, x_hbm, ids_hbm, gain_hbm, w_hbm, x_vmem, ids_vmem, gain_vmem, gain_wide, n_vmem, w_vmem,
                x_sem, small_sem, w_sem, started=None):
    steps, seqs, dim = x_vmem.shape
    drafts = ids_vmem.shape[0]
    cols = w_vmem.shape[0]
    chunks = bounds_of(cols, cfg['sizes'])

    gain_copy = pltpu.make_async_copy(gain_hbm, gain_vmem, small_sem.at[1])
    ids_copy = pltpu.make_async_copy(ids_hbm, ids_vmem, small_sem.at[0])
    x_copies = [pltpu.make_async_copy(x_hbm.at[t], x_vmem.at[t], x_sem.at[t]) for t in range(steps)]
    w_copies = [
        pltpu.make_async_copy(w_hbm.at[pl.ds(start, size)], w_vmem.at[pl.ds(start, size)], w_sem.at[i])
        for i, (start, size) in enumerate(chunks)
    ]
    window = cfg['window']
    for copy in [gain_copy] + x_copies + [ids_copy] + w_copies[:window]:
        copy.start()
    if started is not None:
        started()

    def arrived(i):
        w_copies[i].wait()
        if i + window < len(chunks):
            w_copies[i + window].start()

    groups = [(t, g) for t in range(steps) for g in range(0, seqs, PACKED)]

    def block(t, g, c):
        return x_vmem[t, pl.ds(g, PACKED), pl.ds(c * LANES, LANES)].astype(jnp.float32)

    inv_rms = {}

    def squares(t, g):
        sums = [None] * 4
        for c in range(dim // LANES):
            x = block(t, g, c)
            sums[c % 4] = x * x if sums[c % 4] is None else sums[c % 4] + x * x
        mean = jnp.sum((sums[0] + sums[1]) + (sums[2] + sums[3]), axis=-1, keepdims=True) / dim
        inv_rms[t, g] = lax.rsqrt(mean + NORM_EPS)

    gain_copy.wait()
    gain_wide[...] = gain_vmem[...].astype(jnp.float32)
    for t in range(steps):
        x_copies[t].wait()
        for tt, g in groups:
            if tt == t:
                squares(t, g)
    ids_copy.wait()
    ids = jnp.concatenate(
        [ids_vmem[pl.ds(t, 1), :] for t in range(drafts)] + [jnp.full((1, LANES - drafts * seqs), -1, jnp.int32)],
        axis=1,
    )
    local_ids = ids - me * cols
    arrived(0)
    for c in range(dim // LANES):
        for t, g in groups:
            n = block(t, g, c) * inv_rms[t, g] * gain_wide[pl.ds(c, 1), :]
            n_vmem[pl.ds(t * seqs + g, PACKED), pl.ds(c * LANES, LANES)] = n.astype(jnp.bfloat16)

    carry = (None,) * 4
    pending = []
    for i, (start, size) in enumerate(chunks):
        if i:
            arrived(i)
        first = -(-size // 2 // PACKED) * PACKED
        outs = []
        for begin, part in ((start, first), (start + first, size - first)):
            outs.append((begin, lax.dot_general(
                w_vmem[pl.ds(begin, part), :], n_vmem[...], (((1,), (1,)), ((), ())),
                preferred_element_type=jnp.float32,
            )))
        for begin, tiles in pending:
            carry = stats_of(carry, local_ids, begin, tiles)
        pending = outs
    for begin, tiles in pending:
        carry = stats_of(carry, local_ids, begin, tiles)
    return fold(carry)


def head_kernel(
    cfg, peers,
    x_hbm, ids_hbm, gain_hbm, w_hbm,
    logp_ref, norm_ref, ent_ref,
    own, recv, send_sem, recv_sem, *scratch,
):
    steps, seqs, _ = scratch[0].shape
    drafts = scratch[1].shape[0]
    me = lax.axis_index('tp')
    hops = sorted(range(1, peers), key=lambda hop: -min(hop, peers - hop))
    targets = [lax.rem(me + hop, peers) for hop in hops]
    barrier = pltpu.get_barrier_semaphore()

    def announce():
        for target in targets:
            pl.semaphore_signal(barrier, inc=1, device_id={'tp': target}, device_id_type=pl.DeviceIdType.MESH)

    stats = local_stats(cfg, me, x_hbm, ids_hbm, gain_hbm, w_hbm, *scratch, started=announce)
    own[...] = stats
    recv[:, pl.ds(me, 1), :] = stats[:, None, :]

    pl.semaphore_wait(barrier, peers - 1)
    for target in targets:
        pltpu.make_async_remote_copy(
            src_ref=own, dst_ref=recv.at[:, me], send_sem=send_sem, recv_sem=recv_sem,
            device_id={'tp': target}, device_id_type=pl.DeviceIdType.MESH,
        ).start()
    others = recv.at[:, pl.ds(0, peers - 1)]
    pltpu.make_async_copy(others, others, recv_sem).wait()

    tops, sums, weights, picks = (recv[i] for i in range(4))
    full_top = jnp.max(tops, axis=0, keepdims=True)
    drop = tops - full_top
    scale = jnp.exp(drop)
    full_sum = jnp.sum(scale * sums, axis=0, keepdims=True)
    full_weighted = jnp.sum(scale * (weights + sums * drop), axis=0, keepdims=True)
    full_picked = jnp.sum(picks, axis=0, keepdims=True)
    log_sum = jnp.log(full_sum)
    log_norm = full_top + log_sum
    entropy = log_sum - full_weighted / full_sum
    logp = full_picked - log_norm
    for t in range(steps):
        lanes = slice(t * seqs, (t + 1) * seqs)
        norm_ref[pl.ds(t, 1), :] = log_norm[:, lanes]
        ent_ref[pl.ds(t, 1), :] = entropy[:, lanes]
        if t < drafts:
            logp_ref[pl.ds(t, 1), :] = logp[:, lanes]
    pltpu.make_async_copy(others, others, send_sem).wait()


def store_kernel(*refs):
    count = (len(refs) - 1) // 2
    copies = [pltpu.make_async_copy(refs[i], refs[count + i], refs[-1].at[i]) for i in range(count)]
    for copy in copies:
        copy.start()
    for copy in copies:
        copy.wait()


def solution(mesh):
    peers = mesh.shape['tp']

    def per_device(hidden, draft_ids, norm_gain, head_w):
        seqs, steps, dim = hidden.shape
        drafts = draft_ids.shape[1]
        cols = head_w.shape[1]
        vmem = pl.BlockSpec(memory_space=pltpu.VMEM)
        results = pl.pallas_call(
            functools.partial(head_kernel, CFG, peers),
            out_shape=tuple(pltpu.VMEM((n, seqs), jnp.float32) for n in (drafts, steps, steps)),
            in_specs=[pl.BlockSpec(memory_space=pltpu.HBM)] * 4,
            out_specs=(vmem,) * 3,
            scratch_shapes=[
                pltpu.VMEM((4, LANES), jnp.float32),
                pltpu.VMEM((4, peers, LANES), jnp.float32),
                pltpu.SemaphoreType.DMA,
                pltpu.SemaphoreType.DMA,
            ] + local_scratch(steps, seqs, drafts, dim, cols, len(bounds_of(cols, CFG['sizes']))),
            compiler_params=pltpu.CompilerParams(
                collective_id=0, has_side_effects=True, vmem_limit_bytes=60 * 1024 * 1024
            ),
        )(
            *(
                pltpu.with_memory_space_constraint(a, pltpu.HBM)
                for a in (hidden.transpose(1, 0, 2), draft_ids.T, norm_gain.reshape(dim // LANES, LANES), head_w.T)
            )
        )
        logp, log_norm, entropy = pl.pallas_call(
            store_kernel,
            out_shape=tuple(jax.ShapeDtypeStruct(r.shape, r.dtype) for r in results),
            in_specs=[vmem] * len(results),
            out_specs=(pl.BlockSpec(memory_space=pl.ANY),) * len(results),
            scratch_shapes=[pltpu.SemaphoreType.DMA((len(results),))],
        )(*(pltpu.with_memory_space_constraint(r, pltpu.VMEM) for r in results))
        return logp.T, log_norm.T, entropy.T

    specs_in = (P('dp', None, None), P('dp', None), P(None), P(None, 'tp'))
    specs_out = (P('dp', None), P('dp', None), P('dp', None))
    return jax.shard_map(per_device, mesh=mesh, in_specs=specs_in, out_specs=specs_out, check_vma=False)
```

```python
import functools

import jax
import jax.numpy as jnp
from jax import lax
from jax.experimental import pallas as pl
from jax.experimental.pallas import tpu as pltpu
from jax.sharding import PartitionSpec as P

NORM_EPS = 1e-5
LANES = 128
SUBLANES = 8
PACKED = 16
CFG = {'plan': ((800, (1, 1, 1, 1)), (800, (1, 1, 1, 1)), (400, (1, 1, 1, 1))), 'window': 3}


def pieces_of(total, dim, plan):
    out, start = [], 0
    for rows, cuts in plan:
        rows = min(rows, total - start)
        edges = [dim * cut // sum(cuts) for cut in (sum(cuts[:j]) for j in range(len(cuts) + 1))]
        for low, high in zip(edges, edges[1:]):
            out.append((start, rows, low, high - low, high == dim))
        start += rows
    assert start == total
    return out


def stats_of(carry, local_ids, start, tiles):
    top, exp_sum, weighted, picked = carry
    size, lanes = tiles.shape
    tiles = tiles.reshape(size // SUBLANES, SUBLANES, lanes)
    col_ids = lax.broadcasted_iota(jnp.int32, tiles.shape, 0) * SUBLANES + (
        lax.broadcasted_iota(jnp.int32, tiles.shape, 1) + start
    )
    hit = jnp.sum(jnp.where(col_ids == local_ids[None, :, :lanes], tiles, 0.0), axis=0)
    chunk_top = jnp.max(tiles, axis=0)
    new_top = chunk_top if top is None else jnp.maximum(top, chunk_top)
    shifted = tiles - new_top[None]
    exp_vals = jnp.exp(shifted)
    chunk_sum = jnp.sum(exp_vals, axis=0)
    chunk_weighted = jnp.sum(exp_vals * shifted, axis=0)
    if top is None:
        return new_top, chunk_sum, chunk_weighted, hit
    drop = top - new_top
    scale = jnp.exp(drop)
    return (
        new_top,
        chunk_sum + scale * exp_sum,
        chunk_weighted + scale * (weighted + exp_sum * drop),
        picked + hit,
    )


def fold(carry):
    top, exp_sum, weighted, picked = carry
    all_top = jnp.max(top, axis=0, keepdims=True)
    drop = top - all_top
    scale = jnp.exp(drop)
    rows = [
        all_top,
        jnp.sum(scale * exp_sum, axis=0, keepdims=True),
        jnp.sum(scale * (weighted + exp_sum * drop), axis=0, keepdims=True),
        jnp.sum(picked, axis=0, keepdims=True),
    ]
    stats = jnp.concatenate(rows, axis=0)
    lanes = stats.shape[1]
    if lanes < LANES:
        stats = jnp.concatenate([stats, jnp.zeros((stats.shape[0], LANES - lanes), jnp.float32)], axis=1)
    return stats


def local_scratch(steps, seqs, drafts, dim, cols, pieces):
    return [
        pltpu.VMEM((steps, seqs, dim), jnp.bfloat16),
        pltpu.VMEM((drafts, seqs), jnp.int32),
        pltpu.VMEM((dim // LANES, LANES), jnp.bfloat16),
        pltpu.VMEM((dim // LANES, LANES), jnp.float32),
        pltpu.VMEM((steps * seqs, dim), jnp.bfloat16),
        pltpu.VMEM((cols, dim), jnp.bfloat16),
        pltpu.SemaphoreType.DMA((steps,)),
        pltpu.SemaphoreType.DMA((2,)),
        pltpu.SemaphoreType.DMA((pieces,)),
    ]


def local_stats(cfg, me, x_hbm, ids_hbm, gain_hbm, w_hbm, x_vmem, ids_vmem, gain_vmem, gain_wide, n_vmem, w_vmem,
                x_sem, small_sem, w_sem, started=None):
    steps, seqs, dim = x_vmem.shape
    drafts = ids_vmem.shape[0]
    cols = w_vmem.shape[0]
    chunks = pieces_of(cols, dim, cfg['plan'])

    gain_copy = pltpu.make_async_copy(gain_hbm, gain_vmem, small_sem.at[1])
    ids_copy = pltpu.make_async_copy(ids_hbm, ids_vmem, small_sem.at[0])
    x_copies = [pltpu.make_async_copy(x_hbm.at[t], x_vmem.at[t], x_sem.at[t]) for t in range(steps)]
    w_copies = []
    for i, (start, size, low, depth, _) in enumerate(chunks):
        where = (pl.ds(start, size), pl.ds(low, depth))
        w_copies.append(pltpu.make_async_copy(w_hbm.at[where], w_vmem.at[where], w_sem.at[i]))
    window = cfg['window']
    for copy in [gain_copy] + x_copies + [ids_copy] + w_copies[:window]:
        copy.start()
    if started is not None:
        started()

    def arrived(i):
        w_copies[i].wait()
        if i + window < len(chunks):
            w_copies[i + window].start()

    groups = [(t, g) for t in range(steps) for g in range(0, seqs, PACKED)]

    def block(t, g, c):
        return x_vmem[t, pl.ds(g, PACKED), pl.ds(c * LANES, LANES)].astype(jnp.float32)

    inv_rms = {}

    def squares(t, g):
        sums = [None] * 4
        for c in range(dim // LANES):
            x = block(t, g, c)
            sums[c % 4] = x * x if sums[c % 4] is None else sums[c % 4] + x * x
        mean = jnp.sum((sums[0] + sums[1]) + (sums[2] + sums[3]), axis=-1, keepdims=True) / dim
        inv_rms[t, g] = lax.rsqrt(mean + NORM_EPS)

    gain_copy.wait()
    gain_wide[...] = gain_vmem[...].astype(jnp.float32)
    for t in range(steps):
        x_copies[t].wait()
        for tt, g in groups:
            if tt == t:
                squares(t, g)
    ids_copy.wait()
    ids = jnp.concatenate(
        [ids_vmem[pl.ds(t, 1), :] for t in range(drafts)] + [jnp.full((1, LANES - drafts * seqs), -1, jnp.int32)],
        axis=1,
    )
    local_ids = ids - me * cols
    done = [0]

    def normalise(low, high):
        for c in range(max(low, done[0]) // LANES, high // LANES):
            for t, g in groups:
                n = block(t, g, c) * inv_rms[t, g] * gain_wide[pl.ds(c, 1), :]
                n_vmem[pl.ds(t * seqs + g, PACKED), pl.ds(c * LANES, LANES)] = n.astype(jnp.bfloat16)
        done[0] = max(done[0], high)

    normalise(0, chunks[0][3])
    carry = (None,) * 4
    pending = []
    outs = None
    for i, (start, size, low, depth, last) in enumerate(chunks):
        arrived(i)
        first = -(-size // 2 // PACKED) * PACKED
        terms = [
            (begin, lax.dot_general(
                w_vmem[pl.ds(begin, part), pl.ds(low, depth)], n_vmem[:, pl.ds(low, depth)], (((1,), (1,)), ((), ())),
                preferred_element_type=jnp.float32,
            ))
            for begin, part in ((start, first), (start + first, size - first))
        ]
        if i + 1 < len(chunks) and low + depth < dim:
            normalise(chunks[i + 1][2], chunks[i + 1][2] + chunks[i + 1][3])
        outs = terms if outs is None else [(begin, a + b) for (begin, a), (_, b) in zip(outs, terms)]
        for begin, tiles in pending:
            carry = stats_of(carry, local_ids, begin, tiles)
        pending = []
        if last:
            pending, outs = outs, None
    for begin, tiles in pending:
        carry = stats_of(carry, local_ids, begin, tiles)
    return fold(carry)


def head_kernel(
    cfg, peers,
    x_hbm, ids_hbm, gain_hbm, w_hbm,
    logp_ref, norm_ref, ent_ref,
    own, recv, send_sem, recv_sem, *scratch,
):
    steps, seqs, _ = scratch[0].shape
    drafts = scratch[1].shape[0]
    me = lax.axis_index('tp')
    hops = sorted(range(1, peers), key=lambda hop: -min(hop, peers - hop))
    targets = [lax.rem(me + hop, peers) for hop in hops]
    barrier = pltpu.get_barrier_semaphore()

    def announce():
        for target in targets:
            pl.semaphore_signal(barrier, inc=1, device_id={'tp': target}, device_id_type=pl.DeviceIdType.MESH)

    stats = local_stats(cfg, me, x_hbm, ids_hbm, gain_hbm, w_hbm, *scratch, started=announce)
    own[...] = stats
    recv[:, pl.ds(me, 1), :] = stats[:, None, :]

    pl.semaphore_wait(barrier, peers - 1)
    for target in targets:
        pltpu.make_async_remote_copy(
            src_ref=own, dst_ref=recv.at[:, me], send_sem=send_sem, recv_sem=recv_sem,
            device_id={'tp': target}, device_id_type=pl.DeviceIdType.MESH,
        ).start()
    others = recv.at[:, pl.ds(0, peers - 1)]
    pltpu.make_async_copy(others, others, recv_sem).wait()

    tops, sums, weights, picks = (recv[i] for i in range(4))
    full_top = jnp.max(tops, axis=0, keepdims=True)
    drop = tops - full_top
    scale = jnp.exp(drop)
    full_sum = jnp.sum(scale * sums, axis=0, keepdims=True)
    full_weighted = jnp.sum(scale * (weights + sums * drop), axis=0, keepdims=True)
    full_picked = jnp.sum(picks, axis=0, keepdims=True)
    log_sum = jnp.log(full_sum)
    log_norm = full_top + log_sum
    entropy = log_sum - full_weighted / full_sum
    logp = full_picked - log_norm
    for t in range(steps):
        lanes = slice(t * seqs, (t + 1) * seqs)
        norm_ref[pl.ds(t, 1), :] = log_norm[:, lanes]
        ent_ref[pl.ds(t, 1), :] = entropy[:, lanes]
        if t < drafts:
            logp_ref[pl.ds(t, 1), :] = logp[:, lanes]
    pltpu.make_async_copy(others, others, send_sem).wait()


def store_kernel(*refs):
    count = (len(refs) - 1) // 2
    copies = [pltpu.make_async_copy(refs[i], refs[count + i], refs[-1].at[i]) for i in range(count)]
    for copy in copies:
        copy.start()
    for copy in copies:
        copy.wait()


def solution(mesh):
    peers = mesh.shape['tp']

    def per_device(hidden, draft_ids, norm_gain, head_w):
        seqs, steps, dim = hidden.shape
        drafts = draft_ids.shape[1]
        cols = head_w.shape[1]
        vmem = pl.BlockSpec(memory_space=pltpu.VMEM)
        results = pl.pallas_call(
            functools.partial(head_kernel, CFG, peers),
            out_shape=tuple(pltpu.VMEM((n, seqs), jnp.float32) for n in (drafts, steps, steps)),
            in_specs=[pl.BlockSpec(memory_space=pltpu.HBM)] * 4,
            out_specs=(vmem,) * 3,
            scratch_shapes=[
                pltpu.VMEM((4, LANES), jnp.float32),
                pltpu.VMEM((4, peers, LANES), jnp.float32),
                pltpu.SemaphoreType.DMA,
                pltpu.SemaphoreType.DMA,
            ] + local_scratch(steps, seqs, drafts, dim, cols, len(pieces_of(cols, dim, CFG['plan']))),
            compiler_params=pltpu.CompilerParams(
                collective_id=0, has_side_effects=True, vmem_limit_bytes=60 * 1024 * 1024
            ),
        )(
            *(
                pltpu.with_memory_space_constraint(a, pltpu.HBM)
                for a in (hidden.transpose(1, 0, 2), draft_ids.T, norm_gain.reshape(dim // LANES, LANES), head_w.T)
            )
        )
        logp, log_norm, entropy = pl.pallas_call(
            store_kernel,
            out_shape=tuple(jax.ShapeDtypeStruct(r.shape, r.dtype) for r in results),
            in_specs=[vmem] * len(results),
            out_specs=(pl.BlockSpec(memory_space=pl.ANY),) * len(results),
            scratch_shapes=[pltpu.SemaphoreType.DMA((len(results),))],
        )(*(pltpu.with_memory_space_constraint(r, pltpu.VMEM) for r in results))
        return logp.T, log_norm.T, entropy.T

    specs_in = (P('dp', None, None), P('dp', None), P(None), P(None, 'tp'))
    specs_out = (P('dp', None), P('dp', None), P('dp', None))
    return jax.shard_map(per_device, mesh=mesh, in_specs=specs_in, out_specs=specs_out, check_vma=False)
```

```python
import functools

import jax
import jax.numpy as jnp
from jax import lax
from jax.experimental import pallas as pl
from jax.experimental.pallas import tpu as pltpu
from jax.sharding import PartitionSpec as P

NORM_EPS = 1e-5
LANES = 128
SUBLANES = 8
PACKED = 16
CFG = {'sizes': (400,) * 5}


def bounds_of(total, sizes):
    out, start = [], 0
    for size in sizes:
        size = min(size, total - start)
        if size:
            out.append((start, size))
        start += size
    out.extend((begin, min(sizes[-1], total - begin)) for begin in range(start, total, sizes[-1]))
    return out


def stats_of(carry, local_ids, start, tiles):
    top, exp_sum, weighted, picked = carry
    size, lanes = tiles.shape
    tiles = tiles.reshape(size // SUBLANES, SUBLANES, lanes)
    col_ids = lax.broadcasted_iota(jnp.int32, tiles.shape, 0) * SUBLANES + (
        lax.broadcasted_iota(jnp.int32, tiles.shape, 1) + start
    )
    hit = jnp.sum(jnp.where(col_ids == local_ids[None, :, :lanes], tiles, 0.0), axis=0)
    chunk_top = jnp.max(tiles, axis=0)
    new_top = chunk_top if top is None else jnp.maximum(top, chunk_top)
    shifted = tiles - new_top[None]
    exp_vals = jnp.exp(shifted)
    chunk_sum = jnp.sum(exp_vals, axis=0)
    chunk_weighted = jnp.sum(exp_vals * shifted, axis=0)
    if top is None:
        return new_top, chunk_sum, chunk_weighted, hit
    drop = top - new_top
    scale = jnp.exp(drop)
    return (
        new_top,
        chunk_sum + scale * exp_sum,
        chunk_weighted + scale * (weighted + exp_sum * drop),
        picked + hit,
    )


def fold(carry):
    top, exp_sum, weighted, picked = carry
    all_top = jnp.max(top, axis=0, keepdims=True)
    drop = top - all_top
    scale = jnp.exp(drop)
    rows = [
        all_top,
        jnp.sum(scale * exp_sum, axis=0, keepdims=True),
        jnp.sum(scale * (weighted + exp_sum * drop), axis=0, keepdims=True),
        jnp.sum(picked, axis=0, keepdims=True),
    ]
    stats = jnp.concatenate(rows, axis=0)
    lanes = stats.shape[1]
    if lanes < LANES:
        stats = jnp.concatenate([stats, jnp.zeros((stats.shape[0], LANES - lanes), jnp.float32)], axis=1)
    return stats


def local_scratch(steps, seqs, drafts, dim, cols, pieces):
    return [
        pltpu.VMEM((steps, seqs, dim), jnp.bfloat16),
        pltpu.VMEM((drafts, seqs), jnp.int32),
        pltpu.VMEM((dim // LANES, LANES), jnp.bfloat16),
        pltpu.VMEM((dim // LANES, LANES), jnp.float32),
        pltpu.VMEM((steps * seqs, dim), jnp.bfloat16),
        pltpu.VMEM((cols, dim), jnp.bfloat16),
        pltpu.SemaphoreType.DMA((steps,)),
        pltpu.SemaphoreType.DMA((2,)),
        pltpu.SemaphoreType.DMA((pieces,)),
    ]


def local_stats(cfg, me, x_hbm, ids_hbm, gain_hbm, w_hbm, x_vmem, ids_vmem, gain_vmem, gain_wide, n_vmem, w_vmem,
                x_sem, small_sem, w_sem, announce):
    steps, seqs, dim = x_vmem.shape
    drafts = ids_vmem.shape[0]
    cols = w_vmem.shape[0]
    chunks = bounds_of(cols, cfg['sizes'])

    gain_copy = pltpu.make_async_copy(gain_hbm, gain_vmem, small_sem.at[1])
    ids_copy = pltpu.make_async_copy(ids_hbm, ids_vmem, small_sem.at[0])
    x_copies = [pltpu.make_async_copy(x_hbm.at[t], x_vmem.at[t], x_sem.at[t]) for t in range(steps)]
    w_copies = [
        pltpu.make_async_copy(w_hbm.at[pl.ds(start, size)], w_vmem.at[pl.ds(start, size)], w_sem.at[i])
        for i, (start, size) in enumerate(chunks)
    ]
    for copy in [gain_copy] + x_copies + [ids_copy]:
        copy.start()
    announce(0, 1)
    for copy in w_copies:
        copy.start()
    announce(1, None)

    groups = [(t, g) for t in range(steps) for g in range(0, seqs, PACKED)]

    def block(t, g, c):
        return x_vmem[t, pl.ds(g, PACKED), pl.ds(c * LANES, LANES)].astype(jnp.float32)

    inv_rms = {}

    def squares(t, g):
        sums = [None] * 4
        for c in range(dim // LANES):
            x = block(t, g, c)
            sums[c % 4] = x * x if sums[c % 4] is None else sums[c % 4] + x * x
        mean = jnp.sum((sums[0] + sums[1]) + (sums[2] + sums[3]), axis=-1, keepdims=True) / dim
        inv_rms[t, g] = lax.rsqrt(mean + NORM_EPS)

    gain_copy.wait()
    gain_wide[...] = gain_vmem[...].astype(jnp.float32)
    for t in range(steps):
        x_copies[t].wait()
        for tt, g in groups:
            if tt == t:
                squares(t, g)
    ids_copy.wait()
    ids = jnp.concatenate(
        [ids_vmem[pl.ds(t, 1), :] for t in range(drafts)] + [jnp.full((1, LANES - drafts * seqs), -1, jnp.int32)],
        axis=1,
    )
    local_ids = ids - me * cols
    w_copies[0].wait()
    for c in range(dim // LANES):
        for t, g in groups:
            n = block(t, g, c) * inv_rms[t, g] * gain_wide[pl.ds(c, 1), :]
            n_vmem[pl.ds(t * seqs + g, PACKED), pl.ds(c * LANES, LANES)] = n.astype(jnp.bfloat16)

    carry = (None,) * 4
    pending = []
    for i, (start, size) in enumerate(chunks):
        if i:
            w_copies[i].wait()
        first = -(-size // 2 // PACKED) * PACKED
        outs = []
        for begin, part in ((start, first), (start + first, size - first)):
            outs.append((begin, lax.dot_general(
                w_vmem[pl.ds(begin, part), :], n_vmem[...], (((1,), (1,)), ((), ())),
                preferred_element_type=jnp.float32,
            )))
        for begin, tiles in pending:
            carry = stats_of(carry, local_ids, begin, tiles)
        pending = outs
    for begin, tiles in pending:
        carry = stats_of(carry, local_ids, begin, tiles)
    return fold(carry)


def head_kernel(
    cfg, peers,
    x_hbm, ids_hbm, gain_hbm, w_hbm,
    logp_ref, norm_ref, ent_ref,
    own, recv, send_sem, recv_sem, *scratch,
):
    steps, seqs, _ = scratch[0].shape
    drafts = scratch[1].shape[0]
    me = lax.axis_index('tp')
    hops = sorted(range(1, peers), key=lambda hop: -min(hop, peers - hop))
    targets = [lax.rem(me + hop, peers) for hop in hops]
    barrier = pltpu.get_barrier_semaphore()

    def announce(begin, end):
        for target in targets[begin:end]:
            pl.semaphore_signal(barrier, inc=1, device_id={'tp': target}, device_id_type=pl.DeviceIdType.MESH)

    stats = local_stats(cfg, me, x_hbm, ids_hbm, gain_hbm, w_hbm, *scratch, announce)
    own[...] = stats
    recv[:, pl.ds(me, 1), :] = stats[:, None, :]

    pl.semaphore_wait(barrier, peers - 1)
    for target in targets:
        pltpu.make_async_remote_copy(
            src_ref=own, dst_ref=recv.at[:, me], send_sem=send_sem, recv_sem=recv_sem,
            device_id={'tp': target}, device_id_type=pl.DeviceIdType.MESH,
        ).start()
    others = recv.at[:, pl.ds(0, peers - 1)]
    pltpu.make_async_copy(others, others, recv_sem).wait()

    tops, sums, weights, picks = (recv[i] for i in range(4))
    full_top = jnp.max(tops, axis=0, keepdims=True)
    drop = tops - full_top
    scale = jnp.exp(drop)
    full_sum = jnp.sum(scale * sums, axis=0, keepdims=True)
    full_weighted = jnp.sum(scale * (weights + sums * drop), axis=0, keepdims=True)
    full_picked = jnp.sum(picks, axis=0, keepdims=True)
    log_sum = jnp.log(full_sum)
    log_norm = full_top + log_sum
    entropy = log_sum - full_weighted / full_sum
    logp = full_picked - log_norm
    for t in range(steps):
        lanes = slice(t * seqs, (t + 1) * seqs)
        norm_ref[pl.ds(t, 1), :] = log_norm[:, lanes]
        ent_ref[pl.ds(t, 1), :] = entropy[:, lanes]
        if t < drafts:
            logp_ref[pl.ds(t, 1), :] = logp[:, lanes]
    pltpu.make_async_copy(others, others, send_sem).wait()


def store_kernel(*refs):
    count = (len(refs) - 1) // 2
    copies = [pltpu.make_async_copy(refs[i], refs[count + i], refs[-1].at[i]) for i in range(count)]
    for copy in copies:
        copy.start()
    for copy in copies:
        copy.wait()


def solution(mesh):
    peers = mesh.shape['tp']

    def per_device(hidden, draft_ids, norm_gain, head_w):
        seqs, steps, dim = hidden.shape
        drafts = draft_ids.shape[1]
        cols = head_w.shape[1]
        vmem = pl.BlockSpec(memory_space=pltpu.VMEM)
        results = pl.pallas_call(
            functools.partial(head_kernel, CFG, peers),
            out_shape=tuple(pltpu.VMEM((n, seqs), jnp.float32) for n in (drafts, steps, steps)),
            in_specs=[pl.BlockSpec(memory_space=pltpu.HBM)] * 4,
            out_specs=(vmem,) * 3,
            scratch_shapes=[
                pltpu.VMEM((4, LANES), jnp.float32),
                pltpu.VMEM((4, peers, LANES), jnp.float32),
                pltpu.SemaphoreType.DMA,
                pltpu.SemaphoreType.DMA,
            ] + local_scratch(steps, seqs, drafts, dim, cols, len(bounds_of(cols, CFG['sizes']))),
            compiler_params=pltpu.CompilerParams(
                collective_id=0, has_side_effects=True, vmem_limit_bytes=60 * 1024 * 1024
            ),
        )(
            *(
                pltpu.with_memory_space_constraint(a, pltpu.HBM)
                for a in (hidden.transpose(1, 0, 2), draft_ids.T, norm_gain.reshape(dim // LANES, LANES), head_w.T)
            )
        )
        logp, log_norm, entropy = pl.pallas_call(
            store_kernel,
            out_shape=tuple(jax.ShapeDtypeStruct(r.shape, r.dtype) for r in results),
            in_specs=[vmem] * len(results),
            out_specs=(pl.BlockSpec(memory_space=pl.ANY),) * len(results),
            scratch_shapes=[pltpu.SemaphoreType.DMA((len(results),))],
        )(*(pltpu.with_memory_space_constraint(r, pltpu.VMEM) for r in results))
        return logp.T, log_norm.T, entropy.T

    specs_in = (P('dp', None, None), P('dp', None), P(None), P(None, 'tp'))
    specs_out = (P('dp', None), P('dp', None), P('dp', None))
    return jax.shard_map(per_device, mesh=mesh, in_specs=specs_in, out_specs=specs_out, check_vma=False)
```

```python
import functools

import jax
import jax.numpy as jnp
from jax import lax
from jax.experimental import pallas as pl
from jax.experimental.pallas import tpu as pltpu
from jax.sharding import PartitionSpec as P

NORM_EPS = 1e-5
LANES = 128
SUBLANES = 8
PACKED = 16
CFG = {'sizes': (224, 256, 320, 384, 432, 384)}


def bounds_of(total, sizes):
    out, start = [], 0
    for size in sizes:
        size = min(size, total - start)
        if size:
            out.append((start, size))
        start += size
    out.extend((begin, min(sizes[-1], total - begin)) for begin in range(start, total, sizes[-1]))
    return out


def stats_of(carry, local_ids, start, tiles):
    top, exp_sum, weighted, picked = carry
    size, lanes = tiles.shape
    tiles = tiles.reshape(size // SUBLANES, SUBLANES, lanes)
    col_ids = lax.broadcasted_iota(jnp.int32, tiles.shape, 0) * SUBLANES + (
        lax.broadcasted_iota(jnp.int32, tiles.shape, 1) + start
    )
    hit = jnp.sum(jnp.where(col_ids == local_ids[None, :, :lanes], tiles, 0.0), axis=0)
    chunk_top = jnp.max(tiles, axis=0)
    new_top = chunk_top if top is None else jnp.maximum(top, chunk_top)
    shifted = tiles - new_top[None]
    exp_vals = jnp.exp(shifted)
    chunk_sum = jnp.sum(exp_vals, axis=0)
    chunk_weighted = jnp.sum(exp_vals * shifted, axis=0)
    if top is None:
        return new_top, chunk_sum, chunk_weighted, hit
    drop = top - new_top
    scale = jnp.exp(drop)
    return (
        new_top,
        chunk_sum + scale * exp_sum,
        chunk_weighted + scale * (weighted + exp_sum * drop),
        picked + hit,
    )


def fold(carry, rows, drafts):
    top, exp_sum, weighted, picked = carry
    all_top = jnp.max(top, axis=0, keepdims=True)
    drop = top - all_top
    scale = jnp.exp(drop)
    out = [
        all_top,
        jnp.sum(scale * exp_sum, axis=0, keepdims=True),
        jnp.sum(scale * (weighted + exp_sum * drop), axis=0, keepdims=True),
    ]
    picked = jnp.sum(picked, axis=0, keepdims=True)
    spare = LANES - rows
    for t in range(len(out)):
        lanes = picked[:, t * spare:(t + 1) * spare] if t < drafts else jnp.zeros((1, spare), jnp.float32)
        out[t] = jnp.concatenate([out[t], lanes], axis=1)
    return jnp.concatenate(out, axis=0)


def local_scratch(steps, seqs, drafts, dim, cols, pieces):
    return [
        pltpu.VMEM((steps, seqs, dim), jnp.bfloat16),
        pltpu.VMEM((drafts, seqs), jnp.int32),
        pltpu.VMEM((dim // LANES, LANES), jnp.bfloat16),
        pltpu.VMEM((dim // LANES, LANES), jnp.float32),
        pltpu.VMEM((steps * seqs, dim), jnp.bfloat16),
        pltpu.VMEM((cols, dim), jnp.bfloat16),
        pltpu.SemaphoreType.DMA((steps,)),
        pltpu.SemaphoreType.DMA((2,)),
        pltpu.SemaphoreType.DMA((pieces,)),
    ]


def local_stats(cfg, me, x_hbm, ids_hbm, gain_hbm, w_hbm, x_vmem, ids_vmem, gain_vmem, gain_wide, n_vmem, w_vmem,
                x_sem, small_sem, w_sem, announce):
    steps, seqs, dim = x_vmem.shape
    drafts = ids_vmem.shape[0]
    cols = w_vmem.shape[0]
    chunks = bounds_of(cols, cfg['sizes'])

    gain_copy = pltpu.make_async_copy(gain_hbm, gain_vmem, small_sem.at[1])
    ids_copy = pltpu.make_async_copy(ids_hbm, ids_vmem, small_sem.at[0])
    x_copies = [pltpu.make_async_copy(x_hbm.at[t], x_vmem.at[t], x_sem.at[t]) for t in range(steps)]
    w_copies = [
        pltpu.make_async_copy(w_hbm.at[pl.ds(start, size)], w_vmem.at[pl.ds(start, size)], w_sem.at[i])
        for i, (start, size) in enumerate(chunks)
    ]
    for copy in [gain_copy] + x_copies + [ids_copy]:
        copy.start()
    announce(0, 1)
    for copy in w_copies:
        copy.start()
    announce(1, None)

    groups = [(t, g) for t in range(steps) for g in range(0, seqs, PACKED)]

    def block(t, g, c):
        return x_vmem[t, pl.ds(g, PACKED), pl.ds(c * LANES, LANES)].astype(jnp.float32)

    inv_rms = {}

    def squares(t, g):
        sums = [None] * 4
        for c in range(dim // LANES):
            x = block(t, g, c)
            sums[c % 4] = x * x if sums[c % 4] is None else sums[c % 4] + x * x
        mean = jnp.sum((sums[0] + sums[1]) + (sums[2] + sums[3]), axis=-1, keepdims=True) / dim
        inv_rms[t, g] = lax.rsqrt(mean + NORM_EPS)

    gain_copy.wait()
    gain_wide[...] = gain_vmem[...].astype(jnp.float32)
    for t in range(steps):
        x_copies[t].wait()
        for tt, g in groups:
            if tt == t:
                squares(t, g)
    ids_copy.wait()
    ids = jnp.concatenate(
        [ids_vmem[pl.ds(t, 1), :] for t in range(drafts)] + [jnp.full((1, LANES - drafts * seqs), -1, jnp.int32)],
        axis=1,
    )
    local_ids = ids - me * cols
    w_copies[0].wait()
    for c in range(dim // LANES):
        for t, g in groups:
            n = block(t, g, c) * inv_rms[t, g] * gain_wide[pl.ds(c, 1), :]
            n_vmem[pl.ds(t * seqs + g, PACKED), pl.ds(c * LANES, LANES)] = n.astype(jnp.bfloat16)

    carry = (None,) * 4
    pending = []
    for i, (start, size) in enumerate(chunks):
        if i:
            w_copies[i].wait()
        first = -(-size // 2 // PACKED) * PACKED
        outs = []
        for begin, part in ((start, first), (start + first, size - first)):
            outs.append((begin, lax.dot_general(
                w_vmem[pl.ds(begin, part), :], n_vmem[...], (((1,), (1,)), ((), ())),
                preferred_element_type=jnp.float32,
            )))
        for begin, tiles in pending:
            carry = stats_of(carry, local_ids, begin, tiles)
        pending = outs
    for begin, tiles in pending:
        carry = stats_of(carry, local_ids, begin, tiles)
    return fold(carry, steps * seqs, drafts)


def head_kernel(
    cfg, peers,
    x_hbm, ids_hbm, gain_hbm, w_hbm,
    logp_ref, norm_ref, ent_ref,
    own, recv, send_sem, recv_sem, *scratch,
):
    steps, seqs, _ = scratch[0].shape
    drafts = scratch[1].shape[0]
    me = lax.axis_index('tp')
    targets = [other + jnp.where(other >= me, 1, 0) for other in range(peers - 1)]
    barrier = pltpu.get_barrier_semaphore()

    def announce(begin, end):
        for target in targets[begin:end]:
            pl.semaphore_signal(barrier, inc=1, device_id={'tp': target}, device_id_type=pl.DeviceIdType.MESH)

    stats = local_stats(cfg, me, x_hbm, ids_hbm, gain_hbm, w_hbm, *scratch, announce)
    own[...] = stats
    recv[:, pl.ds(me, 1), :] = stats[:, None, :]

    pl.semaphore_wait(barrier, peers - 1)
    for target in targets:
        pltpu.make_async_remote_copy(
            src_ref=own, dst_ref=recv.at[:, me], send_sem=send_sem, recv_sem=recv_sem,
            device_id={'tp': target}, device_id_type=pl.DeviceIdType.MESH,
        ).start()
    others = recv.at[:, pl.ds(0, peers - 1)]
    pltpu.make_async_copy(others, others, recv_sem).wait()

    tops, sums, weights = (recv[i] for i in range(3))
    full_top = jnp.max(tops, axis=0, keepdims=True)
    drop = tops - full_top
    scale = jnp.exp(drop)
    full_sum = jnp.sum(scale * sums, axis=0, keepdims=True)
    full_weighted = jnp.sum(scale * (weights + sums * drop), axis=0, keepdims=True)
    log_sum = jnp.log(full_sum)
    log_norm = full_top + log_sum
    entropy = log_sum - full_weighted / full_sum
    for t in range(steps):
        lanes = slice(t * seqs, (t + 1) * seqs)
        norm_ref[pl.ds(t, 1), :] = log_norm[:, lanes]
        ent_ref[pl.ds(t, 1), :] = entropy[:, lanes]
        if t < drafts:
            picked = jnp.sum(recv[t], axis=0, keepdims=True)[:, steps * seqs:]
            logp_ref[pl.ds(t, 1), :] = picked - log_norm[:, lanes]
    pltpu.make_async_copy(others, others, send_sem).wait()


def store_kernel(*refs):
    count = (len(refs) - 1) // 2
    copies = [pltpu.make_async_copy(refs[i], refs[count + i], refs[-1].at[i]) for i in range(count)]
    for copy in copies:
        copy.start()
    for copy in copies:
        copy.wait()


def solution(mesh):
    peers = mesh.shape['tp']

    def per_device(hidden, draft_ids, norm_gain, head_w):
        seqs, steps, dim = hidden.shape
        drafts = draft_ids.shape[1]
        cols = head_w.shape[1]
        assert steps >= drafts and seqs == LANES - steps * seqs
        vmem = pl.BlockSpec(memory_space=pltpu.VMEM)
        results = pl.pallas_call(
            functools.partial(head_kernel, CFG, peers),
            out_shape=tuple(pltpu.VMEM((n, seqs), jnp.float32) for n in (drafts, steps, steps)),
            in_specs=[pl.BlockSpec(memory_space=pltpu.HBM)] * 4,
            out_specs=(vmem,) * 3,
            scratch_shapes=[
                pltpu.VMEM((3, LANES), jnp.float32),
                pltpu.VMEM((3, peers, LANES), jnp.float32),
                pltpu.SemaphoreType.DMA,
                pltpu.SemaphoreType.DMA,
            ] + local_scratch(steps, seqs, drafts, dim, cols, len(bounds_of(cols, CFG['sizes']))),
            compiler_params=pltpu.CompilerParams(
                collective_id=0, has_side_effects=True, vmem_limit_bytes=60 * 1024 * 1024
            ),
        )(
            *(
                pltpu.with_memory_space_constraint(a, pltpu.HBM)
                for a in (hidden.transpose(1, 0, 2), draft_ids.T, norm_gain.reshape(dim // LANES, LANES), head_w.T)
            )
        )
        logp, log_norm, entropy = pl.pallas_call(
            store_kernel,
            out_shape=tuple(jax.ShapeDtypeStruct(r.shape, r.dtype) for r in results),
            in_specs=[vmem] * len(results),
            out_specs=(pl.BlockSpec(memory_space=pl.ANY),) * len(results),
            scratch_shapes=[pltpu.SemaphoreType.DMA((len(results),))],
        )(*(pltpu.with_memory_space_constraint(r, pltpu.VMEM) for r in results))
        return logp.T, log_norm.T, entropy.T

    specs_in = (P('dp', None, None), P('dp', None), P(None), P(None, 'tp'))
    specs_out = (P('dp', None), P('dp', None), P('dp', None))
    return jax.shard_map(per_device, mesh=mesh, in_specs=specs_in, out_specs=specs_out, check_vma=False)
```

```python
import functools

import jax
import jax.numpy as jnp
from jax import lax
from jax.experimental import pallas as pl
from jax.experimental.pallas import tpu as pltpu
from jax.sharding import PartitionSpec as P

NORM_EPS = 1e-5
LANES = 128
SUBLANES = 8
PACKED = 16
CFG = {'sizes': (208, 256, 304, 368, 400, 464)}


def bounds_of(total, sizes):
    out, start = [], 0
    for size in sizes:
        size = min(size, total - start)
        if size:
            out.append((start, size))
        start += size
    out.extend((begin, min(sizes[-1], total - begin)) for begin in range(start, total, sizes[-1]))
    return out


def stats_of(carry, local_ids, start, tiles):
    top, exp_sum, weighted, picked = carry
    size, lanes = tiles.shape
    tiles = tiles.reshape(size // SUBLANES, SUBLANES, lanes)
    col_ids = lax.broadcasted_iota(jnp.int32, tiles.shape, 0) * SUBLANES + (
        lax.broadcasted_iota(jnp.int32, tiles.shape, 1) + start
    )
    hit = jnp.sum(jnp.where(col_ids == local_ids[None, :, :lanes], tiles, 0.0), axis=0)
    chunk_top = jnp.max(tiles, axis=0)
    new_top = chunk_top if top is None else jnp.maximum(top, chunk_top)
    shifted = tiles - new_top[None]
    exp_vals = jnp.exp(shifted)
    chunk_sum = jnp.sum(exp_vals, axis=0)
    chunk_weighted = jnp.sum(exp_vals * shifted, axis=0)
    if top is None:
        return new_top, chunk_sum, chunk_weighted, hit
    drop = top - new_top
    scale = jnp.exp(drop)
    return (
        new_top,
        chunk_sum + scale * exp_sum,
        chunk_weighted + scale * (weighted + exp_sum * drop),
        picked + hit,
    )


def fold(carry, rows, drafts):
    top, exp_sum, weighted, picked = carry
    all_top = jnp.max(top, axis=0, keepdims=True)
    drop = top - all_top
    scale = jnp.exp(drop)
    out = [
        all_top,
        jnp.sum(scale * exp_sum, axis=0, keepdims=True),
        jnp.sum(scale * (weighted + exp_sum * drop), axis=0, keepdims=True),
    ]
    picked = jnp.sum(picked, axis=0, keepdims=True)
    spare = LANES - rows
    for t in range(len(out)):
        lanes = picked[:, t * spare:(t + 1) * spare] if t < drafts else jnp.zeros((1, spare), jnp.float32)
        out[t] = jnp.concatenate([out[t], lanes], axis=1)
    return jnp.concatenate(out, axis=0)


def local_scratch(steps, seqs, drafts, dim, cols, pieces):
    return [
        pltpu.VMEM((steps, seqs, dim), jnp.bfloat16),
        pltpu.VMEM((drafts, seqs), jnp.int32),
        pltpu.VMEM((dim // LANES, LANES), jnp.bfloat16),
        pltpu.VMEM((dim // LANES, LANES), jnp.float32),
        pltpu.VMEM((steps * seqs, dim), jnp.bfloat16),
        pltpu.VMEM((cols, dim), jnp.bfloat16),
        pltpu.SemaphoreType.DMA((steps,)),
        pltpu.SemaphoreType.DMA((2,)),
        pltpu.SemaphoreType.DMA((pieces,)),
    ]


def local_stats(cfg, me, x_hbm, ids_hbm, gain_hbm, w_hbm, x_vmem, ids_vmem, gain_vmem, gain_wide, n_vmem, w_vmem,
                x_sem, small_sem, w_sem, announce):
    steps, seqs, dim = x_vmem.shape
    drafts = ids_vmem.shape[0]
    cols = w_vmem.shape[0]
    chunks = bounds_of(cols, cfg['sizes'])

    gain_copy = pltpu.make_async_copy(gain_hbm, gain_vmem, small_sem.at[1])
    ids_copy = pltpu.make_async_copy(ids_hbm, ids_vmem, small_sem.at[0])
    x_copies = [pltpu.make_async_copy(x_hbm.at[t], x_vmem.at[t], x_sem.at[t]) for t in range(steps)]
    w_copies = [
        pltpu.make_async_copy(w_hbm.at[pl.ds(start, size)], w_vmem.at[pl.ds(start, size)], w_sem.at[i])
        for i, (start, size) in enumerate(chunks)
    ]
    for copy in [gain_copy, ids_copy] + x_copies:
        copy.start()
    announce(0, 1)
    for copy in w_copies:
        copy.start()
    announce(1, None)

    groups = [(t, g) for t in range(steps) for g in range(0, seqs, PACKED)]

    def block(t, g, c):
        return x_vmem[t, pl.ds(g, PACKED), pl.ds(c * LANES, LANES)].astype(jnp.float32)

    ids_copy.wait()
    ids = jnp.concatenate(
        [ids_vmem[pl.ds(t, 1), :] for t in range(drafts)] + [jnp.full((1, LANES - drafts * seqs), -1, jnp.int32)],
        axis=1,
    )
    local_ids = ids - me * cols
    gain_copy.wait()
    gain_wide[...] = gain_vmem[...].astype(jnp.float32)
    squares = {}
    for t in range(steps):
        x_copies[t].wait()
        for tt, g in groups:
            if tt == t:
                sums = [None] * 4
                for c in range(dim // LANES):
                    x = block(t, g, c)
                    sums[c % 4] = x * x if sums[c % 4] is None else sums[c % 4] + x * x
                squares[t, g] = (sums[0] + sums[1]) + (sums[2] + sums[3])
    inv_rms = {}
    for key in groups:
        inv_rms[key] = lax.rsqrt(jnp.sum(squares[key], axis=-1, keepdims=True) / dim + NORM_EPS)
    for t, g in groups:
        for c in range(dim // LANES):
            n = block(t, g, c) * inv_rms[t, g] * gain_wide[pl.ds(c, 1), :]
            n_vmem[pl.ds(t * seqs + g, PACKED), pl.ds(c * LANES, LANES)] = n.astype(jnp.bfloat16)

    carry = (None,) * 4
    pending = []
    for i, (start, size) in enumerate(chunks):
        w_copies[i].wait()
        first = -(-size // 2 // PACKED) * PACKED
        outs = []
        for begin, part in ((start, first), (start + first, size - first)):
            outs.append((begin, lax.dot_general(
                w_vmem[pl.ds(begin, part), :], n_vmem[...], (((1,), (1,)), ((), ())),
                preferred_element_type=jnp.float32,
            )))
        for begin, tiles in pending:
            carry = stats_of(carry, local_ids, begin, tiles)
        pending = outs
    for begin, tiles in pending:
        carry = stats_of(carry, local_ids, begin, tiles)
    return fold(carry, steps * seqs, drafts)


def head_kernel(
    cfg, peers,
    x_hbm, ids_hbm, gain_hbm, w_hbm,
    logp_ref, norm_ref, ent_ref,
    own, recv, send_sem, recv_sem, *scratch,
):
    steps, seqs, _ = scratch[0].shape
    drafts = scratch[1].shape[0]
    me = lax.axis_index('tp')
    targets = [other + jnp.where(other >= me, 1, 0) for other in range(peers - 1)]
    barrier = pltpu.get_barrier_semaphore()

    def announce(begin, end):
        for target in targets[begin:end]:
            pl.semaphore_signal(barrier, inc=1, device_id={'tp': target}, device_id_type=pl.DeviceIdType.MESH)

    stats = local_stats(cfg, me, x_hbm, ids_hbm, gain_hbm, w_hbm, *scratch, announce)
    own[...] = stats
    recv[:, pl.ds(me, 1), :] = stats[:, None, :]

    pl.semaphore_wait(barrier, peers - 1)
    for target in targets:
        pltpu.make_async_remote_copy(
            src_ref=own, dst_ref=recv.at[:, me], send_sem=send_sem, recv_sem=recv_sem,
            device_id={'tp': target}, device_id_type=pl.DeviceIdType.MESH,
        ).start()
    others = recv.at[:, pl.ds(0, peers - 1)]
    pltpu.make_async_copy(others, others, recv_sem).wait()

    tops, sums, weights = (recv[i] for i in range(3))
    full_top = jnp.max(tops, axis=0, keepdims=True)
    drop = tops - full_top
    scale = jnp.exp(drop)
    full_sum = jnp.sum(scale * sums, axis=0, keepdims=True)
    full_weighted = jnp.sum(scale * (weights + sums * drop), axis=0, keepdims=True)
    log_sum = jnp.log(full_sum)
    log_norm = full_top + log_sum
    entropy = log_sum - full_weighted / full_sum
    for t in range(steps):
        lanes = slice(t * seqs, (t + 1) * seqs)
        norm_ref[pl.ds(t, 1), :] = log_norm[:, lanes]
        ent_ref[pl.ds(t, 1), :] = entropy[:, lanes]
        if t < drafts:
            picked = jnp.sum(recv[t], axis=0, keepdims=True)[:, steps * seqs:]
            logp_ref[pl.ds(t, 1), :] = picked - log_norm[:, lanes]
    pltpu.make_async_copy(others, others, send_sem).wait()


def store_kernel(*refs):
    count = (len(refs) - 1) // 2
    copies = [pltpu.make_async_copy(refs[i], refs[count + i], refs[-1].at[i]) for i in range(count)]
    for copy in copies:
        copy.start()
    for copy in copies:
        copy.wait()


def solution(mesh):
    peers = mesh.shape['tp']

    def per_device(hidden, draft_ids, norm_gain, head_w):
        seqs, steps, dim = hidden.shape
        drafts = draft_ids.shape[1]
        cols = head_w.shape[1]
        assert steps >= drafts and seqs == LANES - steps * seqs
        vmem = pl.BlockSpec(memory_space=pltpu.VMEM)
        results = pl.pallas_call(
            functools.partial(head_kernel, CFG, peers),
            out_shape=tuple(pltpu.VMEM((n, seqs), jnp.float32) for n in (drafts, steps, steps)),
            in_specs=[pl.BlockSpec(memory_space=pltpu.HBM)] * 4,
            out_specs=(vmem,) * 3,
            scratch_shapes=[
                pltpu.VMEM((3, LANES), jnp.float32),
                pltpu.VMEM((3, peers, LANES), jnp.float32),
                pltpu.SemaphoreType.DMA,
                pltpu.SemaphoreType.DMA,
            ] + local_scratch(steps, seqs, drafts, dim, cols, len(bounds_of(cols, CFG['sizes']))),
            compiler_params=pltpu.CompilerParams(
                collective_id=0, has_side_effects=True, vmem_limit_bytes=60 * 1024 * 1024
            ),
        )(
            *(
                pltpu.with_memory_space_constraint(a, pltpu.HBM)
                for a in (hidden.transpose(1, 0, 2), draft_ids.T, norm_gain.reshape(dim // LANES, LANES), head_w.T)
            )
        )
        logp, log_norm, entropy = pl.pallas_call(
            store_kernel,
            out_shape=tuple(jax.ShapeDtypeStruct(r.shape, r.dtype) for r in results),
            in_specs=[vmem] * len(results),
            out_specs=(pl.BlockSpec(memory_space=pl.ANY),) * len(results),
            scratch_shapes=[pltpu.SemaphoreType.DMA((len(results),))],
        )(*(pltpu.with_memory_space_constraint(r, pltpu.VMEM) for r in results))
        return logp.T, log_norm.T, entropy.T

    specs_in = (P('dp', None, None), P('dp', None), P(None), P(None, 'tp'))
    specs_out = (P('dp', None), P('dp', None), P('dp', None))
    return jax.shard_map(per_device, mesh=mesh, in_specs=specs_in, out_specs=specs_out, check_vma=False)
```

```python
import functools

import jax
import jax.numpy as jnp
from jax import lax
from jax.experimental import pallas as pl
from jax.experimental.pallas import tpu as pltpu
from jax.sharding import PartitionSpec as P

NORM_EPS = 1e-5
LANES = 128
SUBLANES = 8
PACKED = 16
CFG = {'sizes': (240, 320, 400, 416, 368, 256)}


def bounds_of(total, sizes):
    out, start = [], 0
    for size in sizes:
        size = min(size, total - start)
        if size:
            out.append((start, size))
        start += size
    out.extend((begin, min(sizes[-1], total - begin)) for begin in range(start, total, sizes[-1]))
    return out


def stats_of(carry, local_ids, start, tiles):
    top, exp_sum, weighted, picked = carry
    size, lanes = tiles.shape
    tiles = tiles.reshape(size // SUBLANES, SUBLANES, lanes)
    col_ids = lax.broadcasted_iota(jnp.int32, tiles.shape, 0) * SUBLANES + (
        lax.broadcasted_iota(jnp.int32, tiles.shape, 1) + start
    )
    hit = jnp.sum(jnp.where(col_ids == local_ids[None, :, :lanes], tiles, 0.0), axis=0)
    chunk_top = jnp.max(tiles, axis=0)
    new_top = chunk_top if top is None else jnp.maximum(top, chunk_top)
    shifted = tiles - new_top[None]
    exp_vals = jnp.exp(shifted)
    chunk_sum = jnp.sum(exp_vals, axis=0)
    chunk_weighted = jnp.sum(exp_vals * shifted, axis=0)
    if top is None:
        return new_top, chunk_sum, chunk_weighted, hit
    drop = top - new_top
    scale = jnp.exp(drop)
    return (
        new_top,
        chunk_sum + scale * exp_sum,
        chunk_weighted + scale * (weighted + exp_sum * drop),
        picked + hit,
    )


def fold(carry, rows, drafts):
    top, exp_sum, weighted, picked = carry
    all_top = jnp.max(top, axis=0, keepdims=True)
    drop = top - all_top
    scale = jnp.exp(drop)
    out = [
        all_top,
        jnp.sum(scale * exp_sum, axis=0, keepdims=True),
        jnp.sum(scale * (weighted + exp_sum * drop), axis=0, keepdims=True),
    ]
    picked = jnp.sum(picked, axis=0, keepdims=True)
    spare = LANES - rows
    for t in range(len(out)):
        lanes = picked[:, t * spare:(t + 1) * spare] if t < drafts else jnp.zeros((1, spare), jnp.float32)
        out[t] = jnp.concatenate([out[t], lanes], axis=1)
    return jnp.concatenate(out, axis=0)


def local_scratch(steps, seqs, drafts, dim, cols, pieces):
    return [
        pltpu.VMEM((steps, seqs, dim), jnp.bfloat16),
        pltpu.VMEM((drafts, seqs), jnp.int32),
        pltpu.VMEM((dim // LANES, LANES), jnp.bfloat16),
        pltpu.VMEM((dim // LANES, LANES), jnp.float32),
        pltpu.VMEM((steps * seqs, dim), jnp.bfloat16),
        pltpu.VMEM((cols, dim), jnp.bfloat16),
        pltpu.SemaphoreType.DMA((steps,)),
        pltpu.SemaphoreType.DMA((2,)),
        pltpu.SemaphoreType.DMA((pieces,)),
    ]


def local_stats(cfg, me, x_hbm, ids_hbm, gain_hbm, w_hbm, x_vmem, ids_vmem, gain_vmem, gain_wide, n_vmem, w_vmem,
                x_sem, small_sem, w_sem, announce):
    steps, seqs, dim = x_vmem.shape
    drafts = ids_vmem.shape[0]
    cols = w_vmem.shape[0]
    chunks = bounds_of(cols, cfg['sizes'])

    gain_copy = pltpu.make_async_copy(gain_hbm, gain_vmem, small_sem.at[1])
    ids_copy = pltpu.make_async_copy(ids_hbm, ids_vmem, small_sem.at[0])
    x_copies = [pltpu.make_async_copy(x_hbm.at[t], x_vmem.at[t], x_sem.at[t]) for t in range(steps)]
    depths = (pl.ds(0, dim // 2), pl.ds(dim // 2, dim // 2))
    w_copies = []
    for i, (start, size) in enumerate(chunks):
        for depth in depths:
            where = (pl.ds(start, size), depth)
            w_copies.append(pltpu.make_async_copy(w_hbm.at[where], w_vmem.at[where], w_sem.at[len(w_copies)]))
    for copy in [gain_copy, ids_copy] + x_copies:
        copy.start()
    announce(0, 1)
    for copy in w_copies:
        copy.start()
    announce(1, None)

    groups = [(t, g) for t in range(steps) for g in range(0, seqs, PACKED)]

    def block(t, g, c):
        return x_vmem[t, pl.ds(g, PACKED), pl.ds(c * LANES, LANES)].astype(jnp.float32)

    ids_copy.wait()
    ids = jnp.concatenate(
        [ids_vmem[pl.ds(t, 1), :] for t in range(drafts)] + [jnp.full((1, LANES - drafts * seqs), -1, jnp.int32)],
        axis=1,
    )
    local_ids = ids - me * cols
    gain_copy.wait()
    gain_wide[...] = gain_vmem[...].astype(jnp.float32)
    squares = {}
    for t in range(steps):
        x_copies[t].wait()
        for tt, g in groups:
            if tt == t:
                sums = [None] * 4
                for c in range(dim // LANES):
                    x = block(t, g, c)
                    sums[c % 4] = x * x if sums[c % 4] is None else sums[c % 4] + x * x
                squares[t, g] = (sums[0] + sums[1]) + (sums[2] + sums[3])
    inv_rms = {}
    for key in groups:
        inv_rms[key] = lax.rsqrt(jnp.sum(squares[key], axis=-1, keepdims=True) / dim + NORM_EPS)
    for t, g in groups:
        for c in range(dim // LANES):
            n = block(t, g, c) * inv_rms[t, g] * gain_wide[pl.ds(c, 1), :]
            n_vmem[pl.ds(t * seqs + g, PACKED), pl.ds(c * LANES, LANES)] = n.astype(jnp.bfloat16)

    def product(begin, part, depth):
        return lax.dot_general(
            w_vmem[pl.ds(begin, part), depth], n_vmem[:, depth], (((1,), (1,)), ((), ())),
            preferred_element_type=jnp.float32,
        )

    carry = (None,) * 4
    opened = []
    for i in range(len(chunks) + 1):
        if i:
            w_copies[2 * i - 1].wait()
        if i < len(chunks):
            w_copies[2 * i].wait()
        closed = [(begin, part, tiles + product(begin, part, depths[1])) for begin, part, tiles in opened]
        opened = []
        if i < len(chunks):
            start, size = chunks[i]
            first = -(-size // 2 // PACKED) * PACKED
            for begin, part in ((start, first), (start + first, size - first)):
                low, high = (product(begin, part, pl.ds(j * (dim // 4), dim // 4)) for j in range(2))
                opened.append((begin, part, low + high))
        for begin, _, tiles in closed:
            carry = stats_of(carry, local_ids, begin, tiles)
    return fold(carry, steps * seqs, drafts)


def head_kernel(
    cfg, peers,
    x_hbm, ids_hbm, gain_hbm, w_hbm,
    logp_ref, norm_ref, ent_ref,
    own, recv, send_sem, recv_sem, *scratch,
):
    steps, seqs, _ = scratch[0].shape
    drafts = scratch[1].shape[0]
    me = lax.axis_index('tp')
    targets = [other + jnp.where(other >= me, 1, 0) for other in range(peers - 1)]
    barrier = pltpu.get_barrier_semaphore()

    def announce(begin, end):
        for target in targets[begin:end]:
            pl.semaphore_signal(barrier, inc=1, device_id={'tp': target}, device_id_type=pl.DeviceIdType.MESH)

    stats = local_stats(cfg, me, x_hbm, ids_hbm, gain_hbm, w_hbm, *scratch, announce)
    own[...] = stats
    recv[:, pl.ds(me, 1), :] = stats[:, None, :]

    pl.semaphore_wait(barrier, peers - 1)
    for target in targets:
        pltpu.make_async_remote_copy(
            src_ref=own, dst_ref=recv.at[:, me], send_sem=send_sem, recv_sem=recv_sem,
            device_id={'tp': target}, device_id_type=pl.DeviceIdType.MESH,
        ).start()
    others = recv.at[:, pl.ds(0, peers - 1)]
    pltpu.make_async_copy(others, others, recv_sem).wait()

    tops, sums, weights = (recv[i] for i in range(3))
    full_top = jnp.max(tops, axis=0, keepdims=True)
    drop = tops - full_top
    scale = jnp.exp(drop)
    full_sum = jnp.sum(scale * sums, axis=0, keepdims=True)
    full_weighted = jnp.sum(scale * (weights + sums * drop), axis=0, keepdims=True)
    log_sum = jnp.log(full_sum)
    log_norm = full_top + log_sum
    entropy = log_sum - full_weighted / full_sum
    for t in range(steps):
        lanes = slice(t * seqs, (t + 1) * seqs)
        norm_ref[pl.ds(t, 1), :] = log_norm[:, lanes]
        ent_ref[pl.ds(t, 1), :] = entropy[:, lanes]
        if t < drafts:
            picked = jnp.sum(recv[t], axis=0, keepdims=True)[:, steps * seqs:]
            logp_ref[pl.ds(t, 1), :] = picked - log_norm[:, lanes]
    pltpu.make_async_copy(others, others, send_sem).wait()


def store_kernel(*refs):
    count = (len(refs) - 1) // 2
    copies = [pltpu.make_async_copy(refs[i], refs[count + i], refs[-1].at[i]) for i in range(count)]
    for copy in copies:
        copy.start()
    for copy in copies:
        copy.wait()


def solution(mesh):
    peers = mesh.shape['tp']

    def per_device(hidden, draft_ids, norm_gain, head_w):
        seqs, steps, dim = hidden.shape
        drafts = draft_ids.shape[1]
        cols = head_w.shape[1]
        assert steps >= drafts and seqs == LANES - steps * seqs
        vmem = pl.BlockSpec(memory_space=pltpu.VMEM)
        results = pl.pallas_call(
            functools.partial(head_kernel, CFG, peers),
            out_shape=tuple(pltpu.VMEM((n, seqs), jnp.float32) for n in (drafts, steps, steps)),
            in_specs=[pl.BlockSpec(memory_space=pltpu.HBM)] * 4,
            out_specs=(vmem,) * 3,
            scratch_shapes=[
                pltpu.VMEM((3, LANES), jnp.float32),
                pltpu.VMEM((3, peers, LANES), jnp.float32),
                pltpu.SemaphoreType.DMA,
                pltpu.SemaphoreType.DMA,
            ] + local_scratch(steps, seqs, drafts, dim, cols, 2 * len(bounds_of(cols, CFG['sizes']))),
            compiler_params=pltpu.CompilerParams(
                collective_id=0, has_side_effects=True, vmem_limit_bytes=60 * 1024 * 1024
            ),
        )(
            *(
                pltpu.with_memory_space_constraint(a, pltpu.HBM)
                for a in (hidden.transpose(1, 0, 2), draft_ids.T, norm_gain.reshape(dim // LANES, LANES), head_w.T)
            )
        )
        logp, log_norm, entropy = pl.pallas_call(
            store_kernel,
            out_shape=tuple(jax.ShapeDtypeStruct(r.shape, r.dtype) for r in results),
            in_specs=[vmem] * len(results),
            out_specs=(pl.BlockSpec(memory_space=pl.ANY),) * len(results),
            scratch_shapes=[pltpu.SemaphoreType.DMA((len(results),))],
        )(*(pltpu.with_memory_space_constraint(r, pltpu.VMEM) for r in results))
        return logp.T, log_norm.T, entropy.T

    specs_in = (P('dp', None, None), P('dp', None), P(None), P(None, 'tp'))
    specs_out = (P('dp', None), P('dp', None), P('dp', None))
    return jax.shard_map(per_device, mesh=mesh, in_specs=specs_in, out_specs=specs_out, check_vma=False)
```

```python
import functools

import jax
import jax.numpy as jnp
from jax import lax
from jax.experimental import pallas as pl
from jax.experimental.pallas import tpu as pltpu
from jax.sharding import PartitionSpec as P

NORM_EPS = 1e-5
LANES = 128
SUBLANES = 8
PACKED = 16
CFG = {'sizes': (160, 240, 272, 272, 272, 272, 256, 256)}


def bounds_of(total, sizes):
    out, start = [], 0
    for size in sizes:
        size = min(size, total - start)
        if size:
            out.append((start, size))
        start += size
    out.extend((begin, min(sizes[-1], total - begin)) for begin in range(start, total, sizes[-1]))
    return out


def stats_of(carry, local_ids, start, tiles):
    top, exp_sum, weighted, picked = carry
    size, lanes = tiles.shape
    tiles = tiles.reshape(size // SUBLANES, SUBLANES, lanes)
    col_ids = lax.broadcasted_iota(jnp.int32, tiles.shape, 0) * SUBLANES + (
        lax.broadcasted_iota(jnp.int32, tiles.shape, 1) + start
    )
    hit = jnp.sum(jnp.where(col_ids == local_ids[None, :, :lanes], tiles, 0.0), axis=0)
    chunk_top = jnp.max(tiles, axis=0)
    new_top = chunk_top if top is None else jnp.maximum(top, chunk_top)
    shifted = tiles - new_top[None]
    exp_vals = jnp.exp(shifted)
    chunk_sum = jnp.sum(exp_vals, axis=0)
    chunk_weighted = jnp.sum(exp_vals * shifted, axis=0)
    if top is None:
        return new_top, chunk_sum, chunk_weighted, hit
    drop = top - new_top
    scale = jnp.exp(drop)
    return (
        new_top,
        chunk_sum + scale * exp_sum,
        chunk_weighted + scale * (weighted + exp_sum * drop),
        picked + hit,
    )


def fold(carry, rows, drafts):
    top, exp_sum, weighted, picked = carry
    all_top = jnp.max(top, axis=0, keepdims=True)
    drop = top - all_top
    scale = jnp.exp(drop)
    out = [
        all_top,
        jnp.sum(scale * exp_sum, axis=0, keepdims=True),
        jnp.sum(scale * (weighted + exp_sum * drop), axis=0, keepdims=True),
    ]
    picked = jnp.sum(picked, axis=0, keepdims=True)
    spare = LANES - rows
    for t in range(len(out)):
        lanes = picked[:, t * spare:(t + 1) * spare] if t < drafts else jnp.zeros((1, spare), jnp.float32)
        out[t] = jnp.concatenate([out[t], lanes], axis=1)
    return jnp.concatenate(out, axis=0)


def local_scratch(steps, seqs, drafts, dim, cols, pieces):
    return [
        pltpu.VMEM((steps, seqs, dim), jnp.bfloat16),
        pltpu.VMEM((drafts, seqs), jnp.int32),
        pltpu.VMEM((dim // LANES, LANES), jnp.bfloat16),
        pltpu.VMEM((dim // LANES, LANES), jnp.float32),
        pltpu.VMEM((steps * seqs, dim), jnp.bfloat16),
        pltpu.VMEM((cols, dim), jnp.bfloat16),
        pltpu.SemaphoreType.DMA((steps,)),
        pltpu.SemaphoreType.DMA((2,)),
        pltpu.SemaphoreType.DMA((pieces,)),
    ]


def local_stats(cfg, me, x_hbm, ids_hbm, gain_hbm, w_hbm, x_vmem, ids_vmem, gain_vmem, gain_wide, n_vmem, w_vmem,
                x_sem, small_sem, w_sem, announce):
    steps, seqs, dim = x_vmem.shape
    drafts = ids_vmem.shape[0]
    cols = w_vmem.shape[0]
    chunks = bounds_of(cols, cfg['sizes'])

    gain_copy = pltpu.make_async_copy(gain_hbm, gain_vmem, small_sem.at[1])
    ids_copy = pltpu.make_async_copy(ids_hbm, ids_vmem, small_sem.at[0])
    x_copies = [pltpu.make_async_copy(x_hbm.at[t], x_vmem.at[t], x_sem.at[t]) for t in range(steps)]
    depths = (pl.ds(0, dim // 2), pl.ds(dim // 2, dim // 2))
    w_copies = []
    for i, (start, size) in enumerate(chunks):
        for depth in depths:
            where = (pl.ds(start, size), depth)
            w_copies.append(pltpu.make_async_copy(w_hbm.at[where], w_vmem.at[where], w_sem.at[len(w_copies)]))
    for copy in [gain_copy, ids_copy] + x_copies:
        copy.start()
    announce(0, 1)
    for copy in w_copies:
        copy.start()
    announce(1, None)

    groups = [(t, g) for t in range(steps) for g in range(0, seqs, PACKED)]

    def block(t, g, c):
        return x_vmem[t, pl.ds(g, PACKED), pl.ds(c * LANES, LANES)].astype(jnp.float32)

    ids_copy.wait()
    ids = jnp.concatenate(
        [ids_vmem[pl.ds(t, 1), :] for t in range(drafts)] + [jnp.full((1, LANES - drafts * seqs), -1, jnp.int32)],
        axis=1,
    )
    local_ids = ids - me * cols
    gain_copy.wait()
    gain_wide[...] = gain_vmem[...].astype(jnp.float32)
    squares = {}
    for t in range(steps):
        x_copies[t].wait()
        for tt, g in groups:
            if tt == t:
                sums = [None] * 4
                for c in range(dim // LANES):
                    x = block(t, g, c)
                    sums[c % 4] = x * x if sums[c % 4] is None else sums[c % 4] + x * x
                squares[t, g] = (sums[0] + sums[1]) + (sums[2] + sums[3])
    inv_rms = {}
    for key in groups:
        inv_rms[key] = lax.rsqrt(jnp.sum(squares[key], axis=-1, keepdims=True) / dim + NORM_EPS)
    for t, g in groups:
        for c in range(dim // LANES):
            n = block(t, g, c) * inv_rms[t, g] * gain_wide[pl.ds(c, 1), :]
            n_vmem[pl.ds(t * seqs + g, PACKED), pl.ds(c * LANES, LANES)] = n.astype(jnp.bfloat16)

    def product(begin, part, depth):
        return lax.dot_general(
            w_vmem[pl.ds(begin, part), depth], n_vmem[:, depth], (((1,), (1,)), ((), ())),
            preferred_element_type=jnp.float32,
        )

    carry = (None,) * 4
    opened = []
    for i in range(len(chunks) + 1):
        if i:
            w_copies[2 * i - 1].wait()
        if i < len(chunks):
            w_copies[2 * i].wait()
        closed = [(begin, part, tiles + product(begin, part, depths[1])) for begin, part, tiles in opened]
        opened = []
        if i < len(chunks):
            start, size = chunks[i]
            first = -(-size // 2 // PACKED) * PACKED
            for begin, part in ((start, first), (start + first, size - first)):
                low, high = (product(begin, part, pl.ds(j * (dim // 4), dim // 4)) for j in range(2))
                opened.append((begin, part, low + high))
        for begin, _, tiles in closed:
            carry = stats_of(carry, local_ids, begin, tiles)
    return fold(carry, steps * seqs, drafts)


def head_kernel(
    cfg, peers,
    x_hbm, ids_hbm, gain_hbm, w_hbm,
    logp_ref, norm_ref, ent_ref,
    own, recv, send_sem, recv_sem, *scratch,
):
    steps, seqs, _ = scratch[0].shape
    drafts = scratch[1].shape[0]
    me = lax.axis_index('tp')
    targets = [other + jnp.where(other >= me, 1, 0) for other in range(peers - 1)]
    barrier = pltpu.get_barrier_semaphore()

    def announce(begin, end):
        for target in targets[begin:end]:
            pl.semaphore_signal(barrier, inc=1, device_id={'tp': target}, device_id_type=pl.DeviceIdType.MESH)

    stats = local_stats(cfg, me, x_hbm, ids_hbm, gain_hbm, w_hbm, *scratch, announce)
    own[...] = stats
    recv[:, pl.ds(me, 1), :] = stats[:, None, :]

    pl.semaphore_wait(barrier, peers - 1)
    for target in targets:
        pltpu.make_async_remote_copy(
            src_ref=own, dst_ref=recv.at[:, me], send_sem=send_sem, recv_sem=recv_sem,
            device_id={'tp': target}, device_id_type=pl.DeviceIdType.MESH,
        ).start()
    others = recv.at[:, pl.ds(0, peers - 1)]
    pltpu.make_async_copy(others, others, recv_sem).wait()

    tops, sums, weights = (recv[i] for i in range(3))
    full_top = jnp.max(tops, axis=0, keepdims=True)
    drop = tops - full_top
    scale = jnp.exp(drop)
    full_sum = jnp.sum(scale * sums, axis=0, keepdims=True)
    full_weighted = jnp.sum(scale * (weights + sums * drop), axis=0, keepdims=True)
    log_sum = jnp.log(full_sum)
    log_norm = full_top + log_sum
    entropy = log_sum - full_weighted / full_sum
    for t in range(steps):
        lanes = slice(t * seqs, (t + 1) * seqs)
        norm_ref[pl.ds(t, 1), :] = log_norm[:, lanes]
        ent_ref[pl.ds(t, 1), :] = entropy[:, lanes]
        if t < drafts:
            picked = jnp.sum(recv[t], axis=0, keepdims=True)[:, steps * seqs:]
            logp_ref[pl.ds(t, 1), :] = picked - log_norm[:, lanes]
    pltpu.make_async_copy(others, others, send_sem).wait()


def store_kernel(*refs):
    count = (len(refs) - 1) // 2
    copies = [pltpu.make_async_copy(refs[i], refs[count + i], refs[-1].at[i]) for i in range(count)]
    for copy in copies:
        copy.start()
    for copy in copies:
        copy.wait()


def solution(mesh):
    peers = mesh.shape['tp']

    def per_device(hidden, draft_ids, norm_gain, head_w):
        seqs, steps, dim = hidden.shape
        drafts = draft_ids.shape[1]
        cols = head_w.shape[1]
        assert steps >= drafts and seqs == LANES - steps * seqs
        vmem = pl.BlockSpec(memory_space=pltpu.VMEM)
        results = pl.pallas_call(
            functools.partial(head_kernel, CFG, peers),
            out_shape=tuple(pltpu.VMEM((n, seqs), jnp.float32) for n in (drafts, steps, steps)),
            in_specs=[pl.BlockSpec(memory_space=pltpu.HBM)] * 4,
            out_specs=(vmem,) * 3,
            scratch_shapes=[
                pltpu.VMEM((3, LANES), jnp.float32),
                pltpu.VMEM((3, peers, LANES), jnp.float32),
                pltpu.SemaphoreType.DMA,
                pltpu.SemaphoreType.DMA,
            ] + local_scratch(steps, seqs, drafts, dim, cols, 2 * len(bounds_of(cols, CFG['sizes']))),
            compiler_params=pltpu.CompilerParams(
                collective_id=0, has_side_effects=True, vmem_limit_bytes=60 * 1024 * 1024
            ),
        )(
            *(
                pltpu.with_memory_space_constraint(a, pltpu.HBM)
                for a in (hidden.transpose(1, 0, 2), draft_ids.T, norm_gain.reshape(dim // LANES, LANES), head_w.T)
            )
        )
        logp, log_norm, entropy = pl.pallas_call(
            store_kernel,
            out_shape=tuple(jax.ShapeDtypeStruct(r.shape, r.dtype) for r in results),
            in_specs=[vmem] * len(results),
            out_specs=(pl.BlockSpec(memory_space=pl.ANY),) * len(results),
            scratch_shapes=[pltpu.SemaphoreType.DMA((len(results),))],
        )(*(pltpu.with_memory_space_constraint(r, pltpu.VMEM) for r in results))
        return logp.T, log_norm.T, entropy.T

    specs_in = (P('dp', None, None), P('dp', None), P(None), P(None, 'tp'))
    specs_out = (P('dp', None), P('dp', None), P('dp', None))
    return jax.shard_map(per_device, mesh=mesh, in_specs=specs_in, out_specs=specs_out, check_vma=False)
```

```python
import functools

import jax
import jax.numpy as jnp
from jax import lax
from jax.experimental import pallas as pl
from jax.experimental.pallas import tpu as pltpu
from jax.sharding import PartitionSpec as P

NORM_EPS = 1e-5
LANES = 128
SUBLANES = 8
PACKED = 16
CFG = {'sizes': (160, 240, 272, 272, 272, 272, 256, 256)}


def bounds_of(total, sizes):
    out, start = [], 0
    for size in sizes:
        size = min(size, total - start)
        if size:
            out.append((start, size))
        start += size
    out.extend((begin, min(sizes[-1], total - begin)) for begin in range(start, total, sizes[-1]))
    return out


def stats_of(carry, local_ids, start, tiles):
    top, exp_sum, weighted, picked = carry
    size, lanes = tiles.shape
    tiles = tiles.reshape(size // SUBLANES, SUBLANES, lanes)
    col_ids = lax.broadcasted_iota(jnp.int32, tiles.shape, 0) * SUBLANES + (
        lax.broadcasted_iota(jnp.int32, tiles.shape, 1) + start
    )
    hit = jnp.sum(jnp.where(col_ids == local_ids[None, :, :lanes], tiles, 0.0), axis=0)
    chunk_top = jnp.max(tiles, axis=0)
    new_top = chunk_top if top is None else jnp.maximum(top, chunk_top)
    shifted = tiles - new_top[None]
    exp_vals = jnp.exp(shifted)
    chunk_sum = jnp.sum(exp_vals, axis=0)
    chunk_weighted = jnp.sum(exp_vals * shifted, axis=0)
    if top is None:
        return new_top, chunk_sum, chunk_weighted, hit
    drop = top - new_top
    scale = jnp.exp(drop)
    return (
        new_top,
        chunk_sum + scale * exp_sum,
        chunk_weighted + scale * (weighted + exp_sum * drop),
        picked + hit,
    )


def fold(carry, rows, drafts):
    top, exp_sum, weighted, picked = carry
    all_top = jnp.max(top, axis=0, keepdims=True)
    drop = top - all_top
    scale = jnp.exp(drop)
    out = [
        all_top,
        jnp.sum(scale * exp_sum, axis=0, keepdims=True),
        jnp.sum(scale * (weighted + exp_sum * drop), axis=0, keepdims=True),
    ]
    picked = jnp.sum(picked, axis=0, keepdims=True)
    spare = LANES - rows
    for t in range(len(out)):
        lanes = picked[:, t * spare:(t + 1) * spare] if t < drafts else jnp.zeros((1, spare), jnp.float32)
        out[t] = jnp.concatenate([out[t], lanes], axis=1)
    return jnp.concatenate(out, axis=0)


def local_scratch(steps, seqs, drafts, dim, cols, pieces):
    return [
        pltpu.VMEM((steps, seqs, dim), jnp.bfloat16),
        pltpu.VMEM((drafts, seqs), jnp.int32),
        pltpu.VMEM((dim // LANES, LANES), jnp.bfloat16),
        pltpu.VMEM((dim // LANES, LANES), jnp.float32),
        pltpu.VMEM((steps * seqs, dim), jnp.bfloat16),
        pltpu.VMEM((cols, dim), jnp.bfloat16),
        pltpu.SemaphoreType.DMA((steps,)),
        pltpu.SemaphoreType.DMA((2,)),
        pltpu.SemaphoreType.DMA((pieces,)),
    ]


def local_stats(cfg, me, x_hbm, ids_hbm, gain_hbm, w_hbm, x_vmem, ids_vmem, gain_vmem, gain_wide, n_vmem, w_vmem,
                x_sem, small_sem, w_sem, announce):
    steps, seqs, dim = x_vmem.shape
    drafts = ids_vmem.shape[0]
    cols = w_vmem.shape[0]
    chunks = bounds_of(cols, cfg['sizes'])

    gain_copy = pltpu.make_async_copy(gain_hbm, gain_vmem, small_sem.at[1])
    ids_copy = pltpu.make_async_copy(ids_hbm, ids_vmem, small_sem.at[0])
    x_copies = [pltpu.make_async_copy(x_hbm.at[t], x_vmem.at[t], x_sem.at[t]) for t in range(steps)]
    depths = (pl.ds(0, dim // 2), pl.ds(dim // 2, dim // 2))
    w_copies = []
    for i, (start, size) in enumerate(chunks):
        for depth in depths:
            where = (pl.ds(start, size), depth)
            w_copies.append(pltpu.make_async_copy(w_hbm.at[where], w_vmem.at[where], w_sem.at[len(w_copies)]))
    for copy in [gain_copy, ids_copy] + x_copies:
        copy.start()
    announce(0, 1)
    for copy in w_copies:
        copy.start()
    announce(1, None)

    groups = [(t, g) for t in range(steps) for g in range(0, seqs, PACKED)]

    def block(t, g, c):
        return x_vmem[t, pl.ds(g, PACKED), pl.ds(c * LANES, LANES)].astype(jnp.float32)

    ids_copy.wait()
    ids = jnp.concatenate(
        [ids_vmem[pl.ds(t, 1), :] for t in range(drafts)] + [jnp.full((1, LANES - drafts * seqs), -1, jnp.int32)],
        axis=1,
    )
    local_ids = ids - me * cols
    gain_copy.wait()
    gain_wide[...] = gain_vmem[...].astype(jnp.float32)
    squares = {}
    for t in range(steps):
        x_copies[t].wait()
        for tt, g in groups:
            if tt == t:
                sums = [None] * 4
                for c in range(dim // LANES):
                    x = block(t, g, c)
                    sums[c % 4] = x * x if sums[c % 4] is None else sums[c % 4] + x * x
                squares[t, g] = (sums[0] + sums[1]) + (sums[2] + sums[3])
    inv_rms = {}
    for key in groups:
        inv_rms[key] = lax.rsqrt(jnp.sum(squares[key], axis=-1, keepdims=True) / dim + NORM_EPS)
    for t, g in groups:
        for c in range(dim // LANES):
            n = block(t, g, c) * inv_rms[t, g] * gain_wide[pl.ds(c, 1), :]
            n_vmem[pl.ds(t * seqs + g, PACKED), pl.ds(c * LANES, LANES)] = n.astype(jnp.bfloat16)

    def product(begin, part, depth):
        return lax.dot_general(
            w_vmem[pl.ds(begin, part), depth], n_vmem[:, depth], (((1,), (1,)), ((), ())),
            preferred_element_type=jnp.float32,
        )

    carry = (None,) * 4
    opened = []
    for i in range(len(chunks) + 1):
        if i:
            w_copies[2 * i - 1].wait()
        if i < len(chunks):
            w_copies[2 * i].wait()
        closed = [(begin, part, tiles + product(begin, part, depths[1])) for begin, part, tiles in opened]
        opened = []
        if i < len(chunks):
            start, size = chunks[i]
            first = -(-size // 2 // PACKED) * PACKED
            for begin, part in ((start, first), (start + first, size - first)):
                low, high = (product(begin, part, pl.ds(j * (dim // 4), dim // 4)) for j in range(2))
                opened.append((begin, part, low + high))
        for begin, _, tiles in closed:
            carry = stats_of(carry, local_ids, begin, tiles)
    return fold(carry, steps * seqs, drafts)


def head_kernel(
    cfg, peers,
    x_hbm, ids_hbm, gain_hbm, w_hbm,
    logp_ref, norm_ref, ent_ref,
    own, recv, sent, send_sem, recv_sem, *scratch,
):
    steps, seqs, _ = scratch[0].shape
    drafts = scratch[1].shape[0]
    me = lax.axis_index('tp')
    targets = [other + jnp.where(other >= me, 1, 0) for other in range(peers - 1)]
    barrier = pltpu.get_barrier_semaphore()

    def announce(begin, end):
        for target in targets[begin:end]:
            pl.semaphore_signal(barrier, inc=1, device_id={'tp': target}, device_id_type=pl.DeviceIdType.MESH)

    stats = local_stats(cfg, me, x_hbm, ids_hbm, gain_hbm, w_hbm, *scratch, announce)
    own[...] = stats
    slot = pl.ds(pl.multiple_of(me * SUBLANES, SUBLANES), stats.shape[0])
    recv[slot, :] = stats

    pl.semaphore_wait(barrier, peers - 1)
    for target in targets:
        pltpu.make_async_remote_copy(
            src_ref=own, dst_ref=recv.at[slot], send_sem=send_sem, recv_sem=recv_sem,
            device_id={'tp': target}, device_id_type=pl.DeviceIdType.MESH,
        ).start()
    others = sent.at[pl.ds(0, peers - 1)]
    pltpu.make_async_copy(others, others, recv_sem).wait()

    tops, sums, weights = parts = [recv[pl.ds(i, peers, stride=SUBLANES), :] for i in range(3)]
    rows = steps * seqs
    picked = jnp.concatenate([jnp.sum(part, axis=0, keepdims=True) for part in parts[:drafts]], axis=0)[:, rows:]
    full_top = jnp.max(tops, axis=0, keepdims=True)
    drop = tops - full_top
    scale = jnp.exp(drop)
    full_sum = jnp.sum(scale * sums, axis=0, keepdims=True)
    full_weighted = jnp.sum(scale * (weights + sums * drop), axis=0, keepdims=True)
    log_sum = jnp.log(full_sum)
    entropy = log_sum - full_weighted / full_sum

    def by_step(row):
        return jnp.concatenate([row[:, t * seqs:(t + 1) * seqs] for t in range(steps)], axis=0)

    log_norm = by_step(full_top + log_sum)
    norm_ref[...] = log_norm
    ent_ref[...] = by_step(entropy)
    logp_ref[...] = picked - log_norm[:drafts]
    pltpu.make_async_copy(others, others, send_sem).wait()


def store_kernel(*refs):
    count = (len(refs) - 1) // 2
    copies = [pltpu.make_async_copy(refs[i], refs[count + i], refs[-1].at[i]) for i in range(count)]
    for copy in copies:
        copy.start()
    for copy in copies:
        copy.wait()


def solution(mesh):
    peers = mesh.shape['tp']

    def per_device(hidden, draft_ids, norm_gain, head_w):
        seqs, steps, dim = hidden.shape
        drafts = draft_ids.shape[1]
        cols = head_w.shape[1]
        assert steps >= drafts and seqs == LANES - steps * seqs
        vmem = pl.BlockSpec(memory_space=pltpu.VMEM)
        results = pl.pallas_call(
            functools.partial(head_kernel, CFG, peers),
            out_shape=tuple(pltpu.VMEM((n, seqs), jnp.float32) for n in (drafts, steps, steps)),
            in_specs=[pl.BlockSpec(memory_space=pltpu.HBM)] * 4,
            out_specs=(vmem,) * 3,
            scratch_shapes=[
                pltpu.VMEM((3, LANES), jnp.float32),
                pltpu.VMEM((peers * SUBLANES, LANES), jnp.float32),
                pltpu.VMEM((peers, 3, LANES), jnp.float32),
                pltpu.SemaphoreType.DMA,
                pltpu.SemaphoreType.DMA,
            ] + local_scratch(steps, seqs, drafts, dim, cols, 2 * len(bounds_of(cols, CFG['sizes']))),
            compiler_params=pltpu.CompilerParams(
                collective_id=0, has_side_effects=True, vmem_limit_bytes=60 * 1024 * 1024
            ),
        )(
            *(
                pltpu.with_memory_space_constraint(a, pltpu.HBM)
                for a in (hidden.transpose(1, 0, 2), draft_ids.T, norm_gain.reshape(dim // LANES, LANES), head_w.T)
            )
        )
        logp, log_norm, entropy = pl.pallas_call(
            store_kernel,
            out_shape=tuple(jax.ShapeDtypeStruct(r.shape, r.dtype) for r in results),
            in_specs=[vmem] * len(results),
            out_specs=(pl.BlockSpec(memory_space=pl.ANY),) * len(results),
            scratch_shapes=[pltpu.SemaphoreType.DMA((len(results),))],
        )(*(pltpu.with_memory_space_constraint(r, pltpu.VMEM) for r in results))
        return logp.T, log_norm.T, entropy.T

    specs_in = (P('dp', None, None), P('dp', None), P(None), P(None, 'tp'))
    specs_out = (P('dp', None), P('dp', None), P('dp', None))
    return jax.shard_map(per_device, mesh=mesh, in_specs=specs_in, out_specs=specs_out, check_vma=False)
```

```python
import functools

import jax
import jax.numpy as jnp
from jax import lax
from jax.experimental import pallas as pl
from jax.experimental.pallas import tpu as pltpu
from jax.sharding import PartitionSpec as P

NORM_EPS = 1e-5
LANES = 128
SUBLANES = 8
PACKED = 16
CFG = {'sizes': (160, 240, 272, 272, 272, 272, 256, 256)}


def bounds_of(total, sizes):
    out, start = [], 0
    for size in sizes:
        size = min(size, total - start)
        if size:
            out.append((start, size))
        start += size
    out.extend((begin, min(sizes[-1], total - begin)) for begin in range(start, total, sizes[-1]))
    return out


def stats_of(carry, local_ids, start, tiles):
    top, exp_sum, weighted, picked = carry
    size, lanes = tiles.shape
    tiles = tiles.reshape(size // SUBLANES, SUBLANES, lanes)
    col_ids = lax.broadcasted_iota(jnp.int32, tiles.shape, 0) * SUBLANES + (
        lax.broadcasted_iota(jnp.int32, tiles.shape, 1) + start
    )
    hit = jnp.sum(jnp.where(col_ids == local_ids[None, :, :lanes], tiles, 0.0), axis=0)
    chunk_top = jnp.max(tiles, axis=0)
    new_top = chunk_top if top is None else jnp.maximum(top, chunk_top)
    shifted = tiles - new_top[None]
    exp_vals = jnp.exp(shifted)
    chunk_sum = jnp.sum(exp_vals, axis=0)
    chunk_weighted = jnp.sum(exp_vals * shifted, axis=0)
    if top is None:
        return new_top, chunk_sum, chunk_weighted, hit
    drop = top - new_top
    scale = jnp.exp(drop)
    return (
        new_top,
        chunk_sum + scale * exp_sum,
        chunk_weighted + scale * (weighted + exp_sum * drop),
        picked + hit,
    )


def fold(carry, rows, drafts):
    top, exp_sum, weighted, picked = carry
    all_top = jnp.max(top, axis=0, keepdims=True)
    drop = top - all_top
    scale = jnp.exp(drop)
    out = [
        all_top,
        jnp.sum(scale * exp_sum, axis=0, keepdims=True),
        jnp.sum(scale * (weighted + exp_sum * drop), axis=0, keepdims=True),
    ]
    picked = jnp.sum(picked, axis=0, keepdims=True)
    spare = LANES - rows
    for t in range(len(out)):
        lanes = picked[:, t * spare:(t + 1) * spare] if t < drafts else jnp.zeros((1, spare), jnp.float32)
        out[t] = jnp.concatenate([out[t], lanes], axis=1)
    return jnp.concatenate(out, axis=0)


def local_scratch(steps, seqs, drafts, dim, cols, pieces):
    return [
        pltpu.VMEM((steps, seqs, dim), jnp.bfloat16),
        pltpu.VMEM((drafts, seqs), jnp.int32),
        pltpu.VMEM((dim // LANES, LANES), jnp.bfloat16),
        pltpu.VMEM((dim // LANES, LANES), jnp.float32),
        pltpu.VMEM((steps * seqs, dim), jnp.bfloat16),
        pltpu.VMEM((cols, dim), jnp.bfloat16),
        pltpu.SemaphoreType.DMA((steps,)),
        pltpu.SemaphoreType.DMA((2,)),
        pltpu.SemaphoreType.DMA((pieces,)),
    ]


def local_stats(cfg, me, x_hbm, ids_hbm, gain_hbm, w_hbm, x_vmem, ids_vmem, gain_vmem, gain_wide, n_vmem, w_vmem,
                x_sem, small_sem, w_sem, announce):
    steps, seqs, dim = x_vmem.shape
    drafts = ids_vmem.shape[0]
    cols = w_vmem.shape[0]
    chunks = bounds_of(cols, cfg['sizes'])

    gain_copy = pltpu.make_async_copy(gain_hbm, gain_vmem, small_sem.at[1])
    ids_copy = pltpu.make_async_copy(ids_hbm, ids_vmem, small_sem.at[0])
    x_copies = [pltpu.make_async_copy(x_hbm.at[t], x_vmem.at[t], x_sem.at[t]) for t in range(steps)]
    depths = (pl.ds(0, dim // 2), pl.ds(dim // 2, dim // 2))
    w_copies = []
    for i, (start, size) in enumerate(chunks):
        for depth in depths:
            where = (pl.ds(start, size), depth)
            w_copies.append(pltpu.make_async_copy(w_hbm.at[where], w_vmem.at[where], w_sem.at[len(w_copies)]))
    for copy in [gain_copy, ids_copy] + x_copies:
        copy.start()
    announce(0, 1)
    for copy in w_copies:
        copy.start()
    announce(1, None)

    groups = [(t, g) for t in range(steps) for g in range(0, seqs, PACKED)]

    def block(t, g, c):
        return x_vmem[t, pl.ds(g, PACKED), pl.ds(c * LANES, LANES)].astype(jnp.float32)

    ids_copy.wait()
    ids = jnp.concatenate(
        [ids_vmem[pl.ds(t, 1), :] for t in range(drafts)] + [jnp.full((1, LANES - drafts * seqs), -1, jnp.int32)],
        axis=1,
    )
    local_ids = ids - me * cols
    gain_copy.wait()
    gain_wide[...] = gain_vmem[...].astype(jnp.float32)
    squares = {}
    for t in range(steps):
        x_copies[t].wait()
        for tt, g in groups:
            if tt == t:
                sums = [None] * 4
                for c in range(dim // LANES):
                    x = block(t, g, c)
                    sums[c % 4] = x * x if sums[c % 4] is None else sums[c % 4] + x * x
                squares[t, g] = (sums[0] + sums[1]) + (sums[2] + sums[3])
    inv_rms = {}
    for key in groups:
        inv_rms[key] = lax.rsqrt(jnp.sum(squares[key], axis=-1, keepdims=True) / dim + NORM_EPS)
    for t, g in groups:
        for c in range(dim // LANES):
            n = block(t, g, c) * inv_rms[t, g] * gain_wide[pl.ds(c, 1), :]
            n_vmem[pl.ds(t * seqs + g, PACKED), pl.ds(c * LANES, LANES)] = n.astype(jnp.bfloat16)

    def product(begin, part, depth):
        return lax.dot_general(
            w_vmem[pl.ds(begin, part), depth], n_vmem[:, depth], (((1,), (1,)), ((), ())),
            preferred_element_type=jnp.float32,
        )

    carry = (None,) * 4
    opened = []
    for i in range(len(chunks) + 1):
        if i:
            w_copies[2 * i - 1].wait()
        if i < len(chunks):
            w_copies[2 * i].wait()
        closed = [(begin, part, tiles + product(begin, part, depths[1])) for begin, part, tiles in opened]
        opened = []
        if i < len(chunks):
            start, size = chunks[i]
            first = -(-size // 2 // PACKED) * PACKED
            for begin, part in ((start, first), (start + first, size - first)):
                low, high = (product(begin, part, pl.ds(j * (dim // 4), dim // 4)) for j in range(2))
                opened.append((begin, part, low + high))
        for begin, _, tiles in closed:
            carry = stats_of(carry, local_ids, begin, tiles)
    return fold(carry, steps * seqs, drafts)


def head_kernel(
    cfg, peers,
    x_hbm, ids_hbm, gain_hbm, w_hbm,
    logp_ref, norm_ref, ent_ref,
    own, recv, sent, send_sem, recv_sem, *scratch,
):
    steps, seqs, _ = scratch[0].shape
    drafts = scratch[1].shape[0]
    me = lax.axis_index('tp')
    targets = [other + jnp.where(other >= me, 1, 0) for other in range(peers - 1)]
    barrier = pltpu.get_barrier_semaphore()

    def announce(begin, end):
        for target in targets[begin:end]:
            pl.semaphore_signal(barrier, inc=1, device_id={'tp': target}, device_id_type=pl.DeviceIdType.MESH)

    stats = local_stats(cfg, me, x_hbm, ids_hbm, gain_hbm, w_hbm, *scratch, announce)
    own[...] = stats
    slot = pl.ds(pl.multiple_of(me * SUBLANES, SUBLANES), stats.shape[0])
    recv[slot, :] = stats

    pl.semaphore_wait(barrier, peers - 1)
    for target in targets:
        pltpu.make_async_remote_copy(
            src_ref=own, dst_ref=recv.at[slot], send_sem=send_sem, recv_sem=recv_sem,
            device_id={'tp': target}, device_id_type=pl.DeviceIdType.MESH,
        ).start()
    others = sent.at[pl.ds(0, peers - 1)]
    pltpu.make_async_copy(others, others, recv_sem).wait()

    tops, sums, weights = parts = [recv[pl.ds(i, peers, stride=SUBLANES), :] for i in range(3)]
    rows = steps * seqs
    lane = lax.broadcasted_iota(jnp.int32, (1, LANES), 1)
    picked = jnp.zeros((1, LANES), jnp.float32)
    for t in range(drafts):
        turned = pltpu.roll(jnp.sum(parts[t], axis=0, keepdims=True), (t * seqs - rows) % LANES, 1)
        picked = jnp.where((lane >= t * seqs) & (lane < (t + 1) * seqs), turned, picked)
    full_top = jnp.max(tops, axis=0, keepdims=True)
    drop = tops - full_top
    scale = jnp.exp(drop)
    full_sum = jnp.sum(scale * sums, axis=0, keepdims=True)
    full_weighted = jnp.sum(scale * (weights + sums * drop), axis=0, keepdims=True)
    log_sum = jnp.log(full_sum)
    entropy = log_sum - full_weighted / full_sum

    log_norm = full_top + log_sum
    logp = picked - log_norm
    for t in range(steps):
        lanes = slice(t * seqs, (t + 1) * seqs)
        norm_ref[pl.ds(t, 1), :] = log_norm[:, lanes]
        ent_ref[pl.ds(t, 1), :] = entropy[:, lanes]
        if t < drafts:
            logp_ref[pl.ds(t, 1), :] = logp[:, lanes]
    pltpu.make_async_copy(others, others, send_sem).wait()


def store_kernel(*refs):
    count = (len(refs) - 1) // 2
    copies = [pltpu.make_async_copy(refs[i], refs[count + i], refs[-1].at[i]) for i in range(count)]
    for copy in copies:
        copy.start()
    for copy in copies:
        copy.wait()


def solution(mesh):
    peers = mesh.shape['tp']

    def per_device(hidden, draft_ids, norm_gain, head_w):
        seqs, steps, dim = hidden.shape
        drafts = draft_ids.shape[1]
        cols = head_w.shape[1]
        assert steps >= drafts and seqs == LANES - steps * seqs
        vmem = pl.BlockSpec(memory_space=pltpu.VMEM)
        results = pl.pallas_call(
            functools.partial(head_kernel, CFG, peers),
            out_shape=tuple(pltpu.VMEM((n, seqs), jnp.float32) for n in (drafts, steps, steps)),
            in_specs=[pl.BlockSpec(memory_space=pltpu.HBM)] * 4,
            out_specs=(vmem,) * 3,
            scratch_shapes=[
                pltpu.VMEM((3, LANES), jnp.float32),
                pltpu.VMEM((peers * SUBLANES, LANES), jnp.float32),
                pltpu.VMEM((peers, 3, LANES), jnp.float32),
                pltpu.SemaphoreType.DMA,
                pltpu.SemaphoreType.DMA,
            ] + local_scratch(steps, seqs, drafts, dim, cols, 2 * len(bounds_of(cols, CFG['sizes']))),
            compiler_params=pltpu.CompilerParams(
                collective_id=0, has_side_effects=True, vmem_limit_bytes=60 * 1024 * 1024
            ),
        )(
            *(
                pltpu.with_memory_space_constraint(a, pltpu.HBM)
                for a in (hidden.transpose(1, 0, 2), draft_ids.T, norm_gain.reshape(dim // LANES, LANES), head_w.T)
            )
        )
        logp, log_norm, entropy = pl.pallas_call(
            store_kernel,
            out_shape=tuple(jax.ShapeDtypeStruct(r.shape, r.dtype) for r in results),
            in_specs=[vmem] * len(results),
            out_specs=(pl.BlockSpec(memory_space=pl.ANY),) * len(results),
            scratch_shapes=[pltpu.SemaphoreType.DMA((len(results),))],
        )(*(pltpu.with_memory_space_constraint(r, pltpu.VMEM) for r in results))
        return logp.T, log_norm.T, entropy.T

    specs_in = (P('dp', None, None), P('dp', None), P(None), P(None, 'tp'))
    specs_out = (P('dp', None), P('dp', None), P('dp', None))
    return jax.shard_map(per_device, mesh=mesh, in_specs=specs_in, out_specs=specs_out, check_vma=False)
```

```python
import functools

import jax
import jax.numpy as jnp
from jax import lax
from jax.experimental import pallas as pl
from jax.experimental.pallas import tpu as pltpu
from jax.sharding import PartitionSpec as P

NORM_EPS = 1e-5
LANES = 128
SUBLANES = 8
PACKED = 16
CFG = {'sizes': (256, 192, 240, 240, 192, 304, 384, 192), 'cuts': ((4, 4, 4, 4), (4, 6, 6), (4, 4, 4, 4), (6, 6, 4), (10, 6), (6, 6, 4), (4, 6, 6), (6, 10))}


def bounds_of(total, sizes):
    out, start = [], 0
    for size in sizes:
        size = min(size, total - start)
        if size:
            out.append((start, size))
        start += size
    out.extend((begin, min(sizes[-1], total - begin)) for begin in range(start, total, sizes[-1]))
    return out


def stats_of(carry, local_ids, start, tiles):
    top, exp_sum, weighted, picked = carry
    size, lanes = tiles.shape
    tiles = tiles.reshape(size // SUBLANES, SUBLANES, lanes)
    col_ids = lax.broadcasted_iota(jnp.int32, tiles.shape, 0) * SUBLANES + (
        lax.broadcasted_iota(jnp.int32, tiles.shape, 1) + start
    )
    hit = jnp.sum(jnp.where(col_ids == local_ids[None, :, :lanes], tiles, 0.0), axis=0)
    chunk_top = jnp.max(tiles, axis=0)
    new_top = chunk_top if top is None else jnp.maximum(top, chunk_top)
    shifted = tiles - new_top[None]
    exp_vals = jnp.exp(shifted)
    chunk_sum = jnp.sum(exp_vals, axis=0)
    chunk_weighted = jnp.sum(exp_vals * shifted, axis=0)
    if top is None:
        return new_top, chunk_sum, chunk_weighted, hit
    drop = top - new_top
    scale = jnp.exp(drop)
    return (
        new_top,
        chunk_sum + scale * exp_sum,
        chunk_weighted + scale * (weighted + exp_sum * drop),
        picked + hit,
    )


def fold(carry, rows, drafts):
    top, exp_sum, weighted, picked = carry
    all_top = jnp.max(top, axis=0, keepdims=True)
    drop = top - all_top
    scale = jnp.exp(drop)
    out = [
        all_top,
        jnp.sum(scale * exp_sum, axis=0, keepdims=True),
        jnp.sum(scale * (weighted + exp_sum * drop), axis=0, keepdims=True),
    ]
    picked = jnp.sum(picked, axis=0, keepdims=True)
    spare = LANES - rows
    for t in range(len(out)):
        lanes = picked[:, t * spare:(t + 1) * spare] if t < drafts else jnp.zeros((1, spare), jnp.float32)
        out[t] = jnp.concatenate([out[t], lanes], axis=1)
    return jnp.concatenate(out, axis=0)


def local_scratch(steps, seqs, drafts, dim, cols, pieces):
    return [
        pltpu.VMEM((steps, seqs, dim), jnp.bfloat16),
        pltpu.VMEM((drafts, seqs), jnp.int32),
        pltpu.VMEM((dim // LANES, LANES), jnp.bfloat16),
        pltpu.VMEM((dim // LANES, LANES), jnp.float32),
        pltpu.VMEM((steps * seqs, dim), jnp.bfloat16),
        pltpu.VMEM((cols, dim), jnp.bfloat16),
        pltpu.SemaphoreType.DMA((steps,)),
        pltpu.SemaphoreType.DMA((2,)),
        pltpu.SemaphoreType.DMA((pieces,)),
    ]


def local_stats(cfg, me, x_hbm, ids_hbm, gain_hbm, w_hbm, x_vmem, ids_vmem, gain_vmem, gain_wide, n_vmem, w_vmem,
                x_sem, small_sem, w_sem, announce):
    steps, seqs, dim = x_vmem.shape
    drafts = ids_vmem.shape[0]
    cols = w_vmem.shape[0]
    chunks = bounds_of(cols, cfg['sizes'])

    gain_copy = pltpu.make_async_copy(gain_hbm, gain_vmem, small_sem.at[1])
    ids_copy = pltpu.make_async_copy(ids_hbm, ids_vmem, small_sem.at[0])
    x_copies = [pltpu.make_async_copy(x_hbm.at[t], x_vmem.at[t], x_sem.at[t]) for t in range(steps)]
    pieces, w_copies = [], []
    for (start, size), cut in zip(chunks, cfg['cuts']):
        edges = [dim * sum(cut[:j]) // sum(cut) for j in range(len(cut) + 1)]
        pieces.append([pl.ds(low, high - low) for low, high in zip(edges, edges[1:])])
        copies = []
        for depth in pieces[-1]:
            where = (pl.ds(start, size), depth)
            sem = w_sem.at[sum(len(c) for c in w_copies) + len(copies)]
            copies.append(pltpu.make_async_copy(w_hbm.at[where], w_vmem.at[where], sem))
        w_copies.append(copies)
    for copy in [gain_copy, ids_copy] + x_copies:
        copy.start()
    announce(0, 1)
    for copy in sum(w_copies, []):
        copy.start()
    announce(1, None)

    groups = [(t, g) for t in range(steps) for g in range(0, seqs, PACKED)]

    def block(t, g, c):
        return x_vmem[t, pl.ds(g, PACKED), pl.ds(c * LANES, LANES)].astype(jnp.float32)

    ids_copy.wait()
    ids = jnp.concatenate(
        [ids_vmem[pl.ds(t, 1), :] for t in range(drafts)] + [jnp.full((1, LANES - drafts * seqs), -1, jnp.int32)],
        axis=1,
    )
    local_ids = ids - me * cols
    gain_copy.wait()
    gain_wide[...] = gain_vmem[...].astype(jnp.float32)
    squares = {}
    for t in range(steps):
        x_copies[t].wait()
        for tt, g in groups:
            if tt == t:
                sums = [None] * 4
                for c in range(dim // LANES):
                    x = block(t, g, c)
                    sums[c % 4] = x * x if sums[c % 4] is None else sums[c % 4] + x * x
                squares[t, g] = (sums[0] + sums[1]) + (sums[2] + sums[3])
    inv_rms = {}
    for key in groups:
        inv_rms[key] = lax.rsqrt(jnp.sum(squares[key], axis=-1, keepdims=True) / dim + NORM_EPS)
    for t, g in groups:
        for c in range(dim // LANES):
            n = block(t, g, c) * inv_rms[t, g] * gain_wide[pl.ds(c, 1), :]
            n_vmem[pl.ds(t * seqs + g, PACKED), pl.ds(c * LANES, LANES)] = n.astype(jnp.bfloat16)

    def product(begin, part, depth):
        return lax.dot_general(
            w_vmem[pl.ds(begin, part), depth], n_vmem[:, depth], (((1,), (1,)), ((), ())),
            preferred_element_type=jnp.float32,
        )

    carry = (None,) * 4
    opened = []
    for i in range(len(chunks) + 1):
        if i:
            w_copies[i - 1][-1].wait()
        if i < len(chunks):
            w_copies[i][0].wait()
        closed = [(begin, tiles + product(begin, part, pieces[i - 1][-1])) for begin, part, tiles in opened]
        opened = []
        if i < len(chunks):
            start, size = chunks[i]
            first = -(-size // 2 // PACKED) * PACKED
            depth = pieces[i][0].size // 2
            for begin, part in ((start, first), (start + first, size - first)):
                low, high = (product(begin, part, pl.ds(j * depth, depth)) for j in range(2))
                opened.append((begin, part, low + high))
        for begin, tiles in closed:
            carry = stats_of(carry, local_ids, begin, tiles)
        if i < len(chunks):
            for copy, piece in zip(w_copies[i][1:-1], pieces[i][1:-1]):
                copy.wait()
                opened = [(begin, part, tiles + product(begin, part, piece)) for begin, part, tiles in opened]
    return fold(carry, steps * seqs, drafts)


def head_kernel(
    cfg, peers,
    x_hbm, ids_hbm, gain_hbm, w_hbm,
    logp_ref, norm_ref, ent_ref,
    own, recv, sent, send_sem, recv_sem, *scratch,
):
    steps, seqs, _ = scratch[0].shape
    drafts = scratch[1].shape[0]
    me = lax.axis_index('tp')
    targets = [other + jnp.where(other >= me, 1, 0) for other in range(peers - 1)]
    barrier = pltpu.get_barrier_semaphore()

    def announce(begin, end):
        for target in targets[begin:end]:
            pl.semaphore_signal(barrier, inc=1, device_id={'tp': target}, device_id_type=pl.DeviceIdType.MESH)

    stats = local_stats(cfg, me, x_hbm, ids_hbm, gain_hbm, w_hbm, *scratch, announce)
    own[...] = stats
    slot = pl.ds(pl.multiple_of(me * SUBLANES, SUBLANES), stats.shape[0])
    recv[slot, :] = stats

    pl.semaphore_wait(barrier, peers - 1)
    for target in targets:
        pltpu.make_async_remote_copy(
            src_ref=own, dst_ref=recv.at[slot], send_sem=send_sem, recv_sem=recv_sem,
            device_id={'tp': target}, device_id_type=pl.DeviceIdType.MESH,
        ).start()
    others = sent.at[pl.ds(0, peers - 1)]
    pltpu.make_async_copy(others, others, recv_sem).wait()

    tops, sums, weights = parts = [recv[pl.ds(i, peers, stride=SUBLANES), :] for i in range(3)]
    rows = steps * seqs
    lane = lax.broadcasted_iota(jnp.int32, (1, LANES), 1)
    picked = jnp.zeros((1, LANES), jnp.float32)
    for t in range(drafts):
        turned = pltpu.roll(jnp.sum(parts[t], axis=0, keepdims=True), (t * seqs - rows) % LANES, 1)
        picked = jnp.where((lane >= t * seqs) & (lane < (t + 1) * seqs), turned, picked)
    full_top = jnp.max(tops, axis=0, keepdims=True)
    drop = tops - full_top
    scale = jnp.exp(drop)
    full_sum = jnp.sum(scale * sums, axis=0, keepdims=True)
    full_weighted = jnp.sum(scale * (weights + sums * drop), axis=0, keepdims=True)
    log_sum = jnp.log(full_sum)
    entropy = log_sum - full_weighted / full_sum

    log_norm = full_top + log_sum
    logp = picked - log_norm
    for t in range(steps):
        lanes = slice(t * seqs, (t + 1) * seqs)
        norm_ref[pl.ds(t, 1), :] = log_norm[:, lanes]
        ent_ref[pl.ds(t, 1), :] = entropy[:, lanes]
        if t < drafts:
            logp_ref[pl.ds(t, 1), :] = logp[:, lanes]
    pltpu.make_async_copy(others, others, send_sem).wait()


def store_kernel(*refs):
    count = (len(refs) - 1) // 2
    copies = [pltpu.make_async_copy(refs[i], refs[count + i], refs[-1].at[i]) for i in range(count)]
    for copy in copies:
        copy.start()
    for copy in copies:
        copy.wait()


def solution(mesh):
    peers = mesh.shape['tp']

    def per_device(hidden, draft_ids, norm_gain, head_w):
        seqs, steps, dim = hidden.shape
        drafts = draft_ids.shape[1]
        cols = head_w.shape[1]
        assert steps >= drafts and seqs == LANES - steps * seqs
        vmem = pl.BlockSpec(memory_space=pltpu.VMEM)
        results = pl.pallas_call(
            functools.partial(head_kernel, CFG, peers),
            out_shape=tuple(pltpu.VMEM((n, seqs), jnp.float32) for n in (drafts, steps, steps)),
            in_specs=[pl.BlockSpec(memory_space=pltpu.HBM)] * 4,
            out_specs=(vmem,) * 3,
            scratch_shapes=[
                pltpu.VMEM((3, LANES), jnp.float32),
                pltpu.VMEM((peers * SUBLANES, LANES), jnp.float32),
                pltpu.VMEM((peers, 3, LANES), jnp.float32),
                pltpu.SemaphoreType.DMA,
                pltpu.SemaphoreType.DMA,
            ] + local_scratch(steps, seqs, drafts, dim, cols, sum(len(cut) for cut in CFG['cuts'])),
            compiler_params=pltpu.CompilerParams(
                collective_id=0, has_side_effects=True, vmem_limit_bytes=60 * 1024 * 1024
            ),
        )(
            *(
                pltpu.with_memory_space_constraint(a, pltpu.HBM)
                for a in (hidden.transpose(1, 0, 2), draft_ids.T, norm_gain.reshape(dim // LANES, LANES), head_w.T)
            )
        )
        logp, log_norm, entropy = pl.pallas_call(
            store_kernel,
            out_shape=tuple(jax.ShapeDtypeStruct(r.shape, r.dtype) for r in results),
            in_specs=[vmem] * len(results),
            out_specs=(pl.BlockSpec(memory_space=pl.ANY),) * len(results),
            scratch_shapes=[pltpu.SemaphoreType.DMA((len(results),))],
        )(*(pltpu.with_memory_space_constraint(r, pltpu.VMEM) for r in results))
        return logp.T, log_norm.T, entropy.T

    specs_in = (P('dp', None, None), P('dp', None), P(None), P(None, 'tp'))
    specs_out = (P('dp', None), P('dp', None), P('dp', None))
    return jax.shard_map(per_device, mesh=mesh, in_specs=specs_in, out_specs=specs_out, check_vma=False)
```

```python
import functools

import jax
import jax.numpy as jnp
from jax import lax
from jax.experimental import pallas as pl
from jax.experimental.pallas import tpu as pltpu
from jax.sharding import PartitionSpec as P

NORM_EPS = 1e-5
LANES = 128
SUBLANES = 8
PACKED = 16
CFG = {'sizes': (224, 192, 192, 208, 224, 224, 256, 288, 192)}


def bounds_of(total, sizes):
    out, start = [], 0
    for size in sizes:
        size = min(size, total - start)
        if size:
            out.append((start, size))
        start += size
    out.extend((begin, min(sizes[-1], total - begin)) for begin in range(start, total, sizes[-1]))
    return out


def stats_of(carry, local_ids, start, tiles):
    top, exp_sum, weighted, picked = carry
    size, lanes = tiles.shape
    tiles = tiles.reshape(size // SUBLANES, SUBLANES, lanes)
    col_ids = lax.broadcasted_iota(jnp.int32, tiles.shape, 0) * SUBLANES + (
        lax.broadcasted_iota(jnp.int32, tiles.shape, 1) + start
    )
    hit = jnp.sum(jnp.where(col_ids == local_ids[None, :, :lanes], tiles, 0.0), axis=0)
    chunk_top = jnp.max(tiles, axis=0)
    new_top = chunk_top if top is None else jnp.maximum(top, chunk_top)
    shifted = tiles - new_top[None]
    exp_vals = jnp.exp(shifted)
    chunk_sum = jnp.sum(exp_vals, axis=0)
    chunk_weighted = jnp.sum(exp_vals * shifted, axis=0)
    if top is None:
        return new_top, chunk_sum, chunk_weighted, hit
    drop = top - new_top
    scale = jnp.exp(drop)
    return (
        new_top,
        chunk_sum + scale * exp_sum,
        chunk_weighted + scale * (weighted + exp_sum * drop),
        picked + hit,
    )


def fold(carry, rows, drafts):
    top, exp_sum, weighted, picked = carry
    all_top = jnp.max(top, axis=0, keepdims=True)
    drop = top - all_top
    scale = jnp.exp(drop)
    out = [
        all_top,
        jnp.sum(scale * exp_sum, axis=0, keepdims=True),
        jnp.sum(scale * (weighted + exp_sum * drop), axis=0, keepdims=True),
    ]
    picked = jnp.sum(picked, axis=0, keepdims=True)
    spare = LANES - rows
    for t in range(len(out)):
        lanes = picked[:, t * spare:(t + 1) * spare] if t < drafts else jnp.zeros((1, spare), jnp.float32)
        out[t] = jnp.concatenate([out[t], lanes], axis=1)
    return jnp.concatenate(out, axis=0)


def local_scratch(steps, seqs, drafts, dim, cols, pieces):
    return [
        pltpu.VMEM((steps, seqs, dim), jnp.bfloat16),
        pltpu.VMEM((drafts, seqs), jnp.int32),
        pltpu.VMEM((dim // LANES, LANES), jnp.bfloat16),
        pltpu.VMEM((dim // LANES, LANES), jnp.float32),
        pltpu.VMEM((steps * seqs, dim), jnp.bfloat16),
        pltpu.VMEM((cols, dim), jnp.bfloat16),
        pltpu.SemaphoreType.DMA((steps,)),
        pltpu.SemaphoreType.DMA((2,)),
        pltpu.SemaphoreType.DMA((pieces,)),
    ]


def local_stats(cfg, me, x_hbm, ids_hbm, gain_hbm, w_hbm, x_vmem, ids_vmem, gain_vmem, gain_wide, n_vmem, w_vmem,
                x_sem, small_sem, w_sem, announce):
    steps, seqs, dim = x_vmem.shape
    drafts = ids_vmem.shape[0]
    cols = w_vmem.shape[0]
    chunks = bounds_of(cols, cfg['sizes'])

    gain_copy = pltpu.make_async_copy(gain_hbm, gain_vmem, small_sem.at[1])
    ids_copy = pltpu.make_async_copy(ids_hbm, ids_vmem, small_sem.at[0])
    x_copies = [pltpu.make_async_copy(x_hbm.at[t], x_vmem.at[t], x_sem.at[t]) for t in range(steps)]
    depths = (pl.ds(0, dim // 2), pl.ds(dim // 2, dim // 2))
    w_copies = []
    for i, (start, size) in enumerate(chunks):
        for depth in depths:
            where = (pl.ds(start, size), depth)
            w_copies.append(pltpu.make_async_copy(w_hbm.at[where], w_vmem.at[where], w_sem.at[len(w_copies)]))
    for copy in [gain_copy, ids_copy] + x_copies:
        copy.start()
    announce(0, 1)
    for copy in w_copies:
        copy.start()
    announce(1, None)

    groups = [(t, g) for t in range(steps) for g in range(0, seqs, PACKED)]

    def block(t, g, c):
        return x_vmem[t, pl.ds(g, PACKED), pl.ds(c * LANES, LANES)].astype(jnp.float32)

    ids_copy.wait()
    ids = jnp.concatenate(
        [ids_vmem[pl.ds(t, 1), :] for t in range(drafts)] + [jnp.full((1, LANES - drafts * seqs), -1, jnp.int32)],
        axis=1,
    )
    local_ids = ids - me * cols
    gain_copy.wait()
    gain_wide[...] = gain_vmem[...].astype(jnp.float32)
    squares = {}
    for t in range(steps):
        x_copies[t].wait()
        for tt, g in groups:
            if tt == t:
                sums = [None] * 4
                for c in range(dim // LANES):
                    x = block(t, g, c)
                    sums[c % 4] = x * x if sums[c % 4] is None else sums[c % 4] + x * x
                squares[t, g] = (sums[0] + sums[1]) + (sums[2] + sums[3])
    inv_rms = {}
    for key in groups:
        inv_rms[key] = lax.rsqrt(jnp.sum(squares[key], axis=-1, keepdims=True) / dim + NORM_EPS)
    for t, g in groups:
        for c in range(dim // LANES):
            n = block(t, g, c) * inv_rms[t, g] * gain_wide[pl.ds(c, 1), :]
            n_vmem[pl.ds(t * seqs + g, PACKED), pl.ds(c * LANES, LANES)] = n.astype(jnp.bfloat16)

    def product(begin, part, depth):
        return lax.dot_general(
            w_vmem[pl.ds(begin, part), depth], n_vmem[:, depth], (((1,), (1,)), ((), ())),
            preferred_element_type=jnp.float32,
        )

    carry = (None,) * 4
    opened = []
    for i in range(len(chunks) + 1):
        if i:
            w_copies[2 * i - 1].wait()
        if i < len(chunks):
            w_copies[2 * i].wait()
        closed = [(begin, part, tiles + product(begin, part, depths[1])) for begin, part, tiles in opened]
        opened = []
        if i < len(chunks):
            start, size = chunks[i]
            first = -(-size // 2 // PACKED) * PACKED
            for begin, part in ((start, first), (start + first, size - first)):
                low, high = (product(begin, part, pl.ds(j * (dim // 4), dim // 4)) for j in range(2))
                opened.append((begin, part, low + high))
        for begin, _, tiles in closed:
            carry = stats_of(carry, local_ids, begin, tiles)
    return fold(carry, steps * seqs, drafts)


def head_kernel(
    cfg, peers,
    x_hbm, ids_hbm, gain_hbm, w_hbm,
    logp_ref, norm_ref, ent_ref,
    own, recv, sent, send_sem, recv_sem, *scratch,
):
    steps, seqs, _ = scratch[0].shape
    drafts = scratch[1].shape[0]
    me = lax.axis_index('tp')
    targets = [other + jnp.where(other >= me, 1, 0) for other in range(peers - 1)]
    barrier = pltpu.get_barrier_semaphore()

    def announce(begin, end):
        for target in targets[begin:end]:
            pl.semaphore_signal(barrier, inc=1, device_id={'tp': target}, device_id_type=pl.DeviceIdType.MESH)

    stats = local_stats(cfg, me, x_hbm, ids_hbm, gain_hbm, w_hbm, *scratch, announce)
    own[...] = stats
    slot = pl.ds(pl.multiple_of(me * SUBLANES, SUBLANES), stats.shape[0])
    recv[slot, :] = stats

    pl.semaphore_wait(barrier, peers - 1)
    for target in targets:
        pltpu.make_async_remote_copy(
            src_ref=own, dst_ref=recv.at[slot], send_sem=send_sem, recv_sem=recv_sem,
            device_id={'tp': target}, device_id_type=pl.DeviceIdType.MESH,
        ).start()
    others = sent.at[pl.ds(0, peers - 1)]
    pltpu.make_async_copy(others, others, recv_sem).wait()

    tops, sums, weights = parts = [recv[pl.ds(i, peers, stride=SUBLANES), :] for i in range(3)]
    rows = steps * seqs
    lane = lax.broadcasted_iota(jnp.int32, (1, LANES), 1)
    picked = jnp.zeros((1, LANES), jnp.float32)
    for t in range(drafts):
        turned = pltpu.roll(jnp.sum(parts[t], axis=0, keepdims=True), (t * seqs - rows) % LANES, 1)
        picked = jnp.where((lane >= t * seqs) & (lane < (t + 1) * seqs), turned, picked)
    full_top = jnp.max(tops, axis=0, keepdims=True)
    drop = tops - full_top
    scale = jnp.exp(drop)
    full_sum = jnp.sum(scale * sums, axis=0, keepdims=True)
    full_weighted = jnp.sum(scale * (weights + sums * drop), axis=0, keepdims=True)
    log_sum = jnp.log(full_sum)
    entropy = log_sum - full_weighted / full_sum

    log_norm = full_top + log_sum
    logp = picked - log_norm
    for t in range(steps):
        lanes = slice(t * seqs, (t + 1) * seqs)
        norm_ref[pl.ds(t, 1), :] = log_norm[:, lanes]
        ent_ref[pl.ds(t, 1), :] = entropy[:, lanes]
        if t < drafts:
            logp_ref[pl.ds(t, 1), :] = logp[:, lanes]
    pltpu.make_async_copy(others, others, send_sem).wait()


def store_kernel(*refs):
    count = (len(refs) - 1) // 2
    copies = [pltpu.make_async_copy(refs[i], refs[count + i], refs[-1].at[i]) for i in range(count)]
    for copy in copies:
        copy.start()
    for copy in copies:
        copy.wait()


def solution(mesh):
    peers = mesh.shape['tp']

    def per_device(hidden, draft_ids, norm_gain, head_w):
        seqs, steps, dim = hidden.shape
        drafts = draft_ids.shape[1]
        cols = head_w.shape[1]
        assert steps >= drafts and seqs == LANES - steps * seqs
        vmem = pl.BlockSpec(memory_space=pltpu.VMEM)
        results = pl.pallas_call(
            functools.partial(head_kernel, CFG, peers),
            out_shape=tuple(pltpu.VMEM((n, seqs), jnp.float32) for n in (drafts, steps, steps)),
            in_specs=[pl.BlockSpec(memory_space=pltpu.HBM)] * 4,
            out_specs=(vmem,) * 3,
            scratch_shapes=[
                pltpu.VMEM((3, LANES), jnp.float32),
                pltpu.VMEM((peers * SUBLANES, LANES), jnp.float32),
                pltpu.VMEM((peers, 3, LANES), jnp.float32),
                pltpu.SemaphoreType.DMA,
                pltpu.SemaphoreType.DMA,
            ] + local_scratch(steps, seqs, drafts, dim, cols, 2 * len(bounds_of(cols, CFG['sizes']))),
            compiler_params=pltpu.CompilerParams(
                collective_id=0, has_side_effects=True, vmem_limit_bytes=60 * 1024 * 1024
            ),
        )(
            *(
                pltpu.with_memory_space_constraint(a, pltpu.HBM)
                for a in (hidden.transpose(1, 0, 2), draft_ids.T, norm_gain.reshape(dim // LANES, LANES), head_w.T)
            )
        )
        logp, log_norm, entropy = pl.pallas_call(
            store_kernel,
            out_shape=tuple(jax.ShapeDtypeStruct(r.shape, r.dtype) for r in results),
            in_specs=[vmem] * len(results),
            out_specs=(pl.BlockSpec(memory_space=pl.ANY),) * len(results),
            scratch_shapes=[pltpu.SemaphoreType.DMA((len(results),))],
        )(*(pltpu.with_memory_space_constraint(r, pltpu.VMEM) for r in results))
        return logp.T, log_norm.T, entropy.T

    specs_in = (P('dp', None, None), P('dp', None), P(None), P(None, 'tp'))
    specs_out = (P('dp', None), P('dp', None), P('dp', None))
    return jax.shard_map(per_device, mesh=mesh, in_specs=specs_in, out_specs=specs_out, check_vma=False)
```

```python
import functools

import jax
import jax.numpy as jnp
from jax import lax
from jax.experimental import pallas as pl
from jax.experimental.pallas import tpu as pltpu
from jax.sharding import PartitionSpec as P

NORM_EPS = 1e-5
LANES = 128
SUBLANES = 8
PACKED = 16
CFG = {'sizes': (144, 224, 272, 288, 288, 288, 272, 224)}


def bounds_of(total, sizes):
    out, start = [], 0
    for size in sizes:
        size = min(size, total - start)
        if size:
            out.append((start, size))
        start += size
    out.extend((begin, min(sizes[-1], total - begin)) for begin in range(start, total, sizes[-1]))
    return out


def stats_of(carry, local_ids, start, tiles):
    top, exp_sum, weighted, picked = carry
    size, lanes = tiles.shape
    tiles = tiles.reshape(size // SUBLANES, SUBLANES, lanes)
    col_ids = lax.broadcasted_iota(jnp.int32, tiles.shape, 0) * SUBLANES + (
        lax.broadcasted_iota(jnp.int32, tiles.shape, 1) + start
    )
    hit = jnp.sum(jnp.where(col_ids == local_ids[None, :, :lanes], tiles, 0.0), axis=0)
    chunk_top = jnp.max(tiles, axis=0)
    new_top = chunk_top if top is None else jnp.maximum(top, chunk_top)
    shifted = tiles - new_top[None]
    exp_vals = jnp.exp(shifted)
    chunk_sum = jnp.sum(exp_vals, axis=0)
    chunk_weighted = jnp.sum(exp_vals * shifted, axis=0)
    if top is None:
        return new_top, chunk_sum, chunk_weighted, hit
    drop = top - new_top
    scale = jnp.exp(drop)
    return (
        new_top,
        chunk_sum + scale * exp_sum,
        chunk_weighted + scale * (weighted + exp_sum * drop),
        picked + hit,
    )


def fold(carry, rows, drafts):
    top, exp_sum, weighted, picked = carry
    all_top = jnp.max(top, axis=0, keepdims=True)
    drop = top - all_top
    scale = jnp.exp(drop)
    out = [
        all_top,
        jnp.sum(scale * exp_sum, axis=0, keepdims=True),
        jnp.sum(scale * (weighted + exp_sum * drop), axis=0, keepdims=True),
    ]
    picked = jnp.sum(picked, axis=0, keepdims=True)
    spare = LANES - rows
    for t in range(len(out)):
        lanes = picked[:, t * spare:(t + 1) * spare] if t < drafts else jnp.zeros((1, spare), jnp.float32)
        out[t] = jnp.concatenate([out[t], lanes], axis=1)
    return jnp.concatenate(out, axis=0)


def local_scratch(steps, seqs, drafts, dim, cols, pieces):
    return [
        pltpu.VMEM((steps, seqs, dim), jnp.bfloat16),
        pltpu.VMEM((drafts, seqs), jnp.int32),
        pltpu.VMEM((dim // LANES, LANES), jnp.bfloat16),
        pltpu.VMEM((dim // LANES, LANES), jnp.float32),
        pltpu.VMEM((steps * seqs, dim), jnp.bfloat16),
        pltpu.VMEM((cols, dim), jnp.bfloat16),
        pltpu.SemaphoreType.DMA((steps,)),
        pltpu.SemaphoreType.DMA((2,)),
        pltpu.SemaphoreType.DMA((pieces,)),
    ]


def local_stats(cfg, me, x_hbm, ids_hbm, gain_hbm, w_hbm, x_vmem, ids_vmem, gain_vmem, gain_wide, n_vmem, w_vmem,
                x_sem, small_sem, w_sem, announce):
    steps, seqs, dim = x_vmem.shape
    drafts = ids_vmem.shape[0]
    cols = w_vmem.shape[0]
    chunks = bounds_of(cols, cfg['sizes'])

    gain_copy = pltpu.make_async_copy(gain_hbm, gain_vmem, small_sem.at[1])
    ids_copy = pltpu.make_async_copy(ids_hbm, ids_vmem, small_sem.at[0])
    x_copies = [pltpu.make_async_copy(x_hbm.at[t], x_vmem.at[t], x_sem.at[t]) for t in range(steps)]
    depths = (pl.ds(0, dim // 2), pl.ds(dim // 2, dim // 2))
    w_copies = []
    for i, (start, size) in enumerate(chunks):
        for depth in depths:
            where = (pl.ds(start, size), depth)
            w_copies.append(pltpu.make_async_copy(w_hbm.at[where], w_vmem.at[where], w_sem.at[len(w_copies)]))
    for copy in [gain_copy, ids_copy] + x_copies:
        copy.start()
    announce(0, 1)
    for copy in w_copies:
        copy.start()
    announce(1, None)

    groups = [(t, g) for t in range(steps) for g in range(0, seqs, PACKED)]

    def block(t, g, c):
        return x_vmem[t, pl.ds(g, PACKED), pl.ds(c * LANES, LANES)].astype(jnp.float32)

    ids_copy.wait()
    ids = jnp.concatenate(
        [ids_vmem[pl.ds(t, 1), :] for t in range(drafts)] + [jnp.full((1, LANES - drafts * seqs), -1, jnp.int32)],
        axis=1,
    )
    local_ids = ids - me * cols
    gain_copy.wait()
    gain_wide[...] = gain_vmem[...].astype(jnp.float32)
    squares = {}
    for t in range(steps):
        x_copies[t].wait()
        for tt, g in groups:
            if tt == t:
                sums = [None] * 4
                for c in range(dim // LANES):
                    x = block(t, g, c)
                    sums[c % 4] = x * x if sums[c % 4] is None else sums[c % 4] + x * x
                squares[t, g] = (sums[0] + sums[1]) + (sums[2] + sums[3])
    inv_rms = {}
    for key in groups:
        inv_rms[key] = lax.rsqrt(jnp.sum(squares[key], axis=-1, keepdims=True) / dim + NORM_EPS)
    for t, g in groups:
        for c in range(dim // LANES):
            n = block(t, g, c) * inv_rms[t, g] * gain_wide[pl.ds(c, 1), :]
            n_vmem[pl.ds(t * seqs + g, PACKED), pl.ds(c * LANES, LANES)] = n.astype(jnp.bfloat16)

    def product(begin, part, depth):
        return lax.dot_general(
            w_vmem[pl.ds(begin, part), depth], n_vmem[:, depth], (((1,), (1,)), ((), ())),
            preferred_element_type=jnp.float32,
        )

    carry = (None,) * 4
    opened = []
    for i in range(len(chunks) + 1):
        if i:
            w_copies[2 * i - 1].wait()
        if i < len(chunks):
            w_copies[2 * i].wait()
        closed = [(begin, part, tiles + product(begin, part, depths[1])) for begin, part, tiles in opened]
        opened = []
        if i < len(chunks):
            start, size = chunks[i]
            first = -(-size // 2 // PACKED) * PACKED
            for begin, part in ((start, first), (start + first, size - first)):
                low, high = (product(begin, part, pl.ds(j * (dim // 4), dim // 4)) for j in range(2))
                opened.append((begin, part, low + high))
        for begin, _, tiles in closed:
            carry = stats_of(carry, local_ids, begin, tiles)
    return fold(carry, steps * seqs, drafts)


def head_kernel(
    cfg, peers,
    x_hbm, ids_hbm, gain_hbm, w_hbm,
    logp_ref, norm_ref, ent_ref,
    own, recv, sent, send_sem, recv_sem, *scratch,
):
    steps, seqs, _ = scratch[0].shape
    drafts = scratch[1].shape[0]
    me = lax.axis_index('tp')
    targets = [other + jnp.where(other >= me, 1, 0) for other in range(peers - 1)]
    barrier = pltpu.get_barrier_semaphore()

    def announce(begin, end):
        for target in targets[begin:end]:
            pl.semaphore_signal(barrier, inc=1, device_id={'tp': target}, device_id_type=pl.DeviceIdType.MESH)

    stats = local_stats(cfg, me, x_hbm, ids_hbm, gain_hbm, w_hbm, *scratch, announce)
    own[...] = stats
    slot = pl.ds(pl.multiple_of(me * SUBLANES, SUBLANES), stats.shape[0])
    recv[slot, :] = stats

    pl.semaphore_wait(barrier, peers - 1)
    for target in targets:
        pltpu.make_async_remote_copy(
            src_ref=own, dst_ref=recv.at[slot], send_sem=send_sem, recv_sem=recv_sem,
            device_id={'tp': target}, device_id_type=pl.DeviceIdType.MESH,
        ).start()
    others = sent.at[pl.ds(0, peers - 1)]
    pltpu.make_async_copy(others, others, recv_sem).wait()

    tops, sums, weights = parts = [recv[pl.ds(i, peers, stride=SUBLANES), :] for i in range(3)]
    rows = steps * seqs
    lane = lax.broadcasted_iota(jnp.int32, (1, LANES), 1)
    picked = jnp.zeros((1, LANES), jnp.float32)
    for t in range(drafts):
        turned = pltpu.roll(jnp.sum(parts[t], axis=0, keepdims=True), (t * seqs - rows) % LANES, 1)
        picked = jnp.where((lane >= t * seqs) & (lane < (t + 1) * seqs), turned, picked)
    full_top = jnp.max(tops, axis=0, keepdims=True)
    drop = tops - full_top
    scale = jnp.exp(drop)
    full_sum = jnp.sum(scale * sums, axis=0, keepdims=True)
    full_weighted = jnp.sum(scale * (weights + sums * drop), axis=0, keepdims=True)
    log_sum = jnp.log(full_sum)
    entropy = log_sum - full_weighted / full_sum

    log_norm = full_top + log_sum
    logp = picked - log_norm
    for t in range(steps):
        lanes = slice(t * seqs, (t + 1) * seqs)
        norm_ref[pl.ds(t, 1), :] = log_norm[:, lanes]
        ent_ref[pl.ds(t, 1), :] = entropy[:, lanes]
        if t < drafts:
            logp_ref[pl.ds(t, 1), :] = logp[:, lanes]
    pltpu.make_async_copy(others, others, send_sem).wait()


def store_kernel(*refs):
    count = (len(refs) - 1) // 2
    copies = [pltpu.make_async_copy(refs[i], refs[count + i], refs[-1].at[i]) for i in range(count)]
    for copy in copies:
        copy.start()
    for copy in copies:
        copy.wait()


def solution(mesh):
    peers = mesh.shape['tp']

    def per_device(hidden, draft_ids, norm_gain, head_w):
        seqs, steps, dim = hidden.shape
        drafts = draft_ids.shape[1]
        cols = head_w.shape[1]
        assert steps >= drafts and seqs == LANES - steps * seqs
        vmem = pl.BlockSpec(memory_space=pltpu.VMEM)
        results = pl.pallas_call(
            functools.partial(head_kernel, CFG, peers),
            out_shape=tuple(pltpu.VMEM((n, seqs), jnp.float32) for n in (drafts, steps, steps)),
            in_specs=[pl.BlockSpec(memory_space=pltpu.HBM)] * 4,
            out_specs=(vmem,) * 3,
            scratch_shapes=[
                pltpu.VMEM((3, LANES), jnp.float32),
                pltpu.VMEM((peers * SUBLANES, LANES), jnp.float32),
                pltpu.VMEM((peers, 3, LANES), jnp.float32),
                pltpu.SemaphoreType.DMA,
                pltpu.SemaphoreType.DMA,
            ] + local_scratch(steps, seqs, drafts, dim, cols, 2 * len(bounds_of(cols, CFG['sizes']))),
            compiler_params=pltpu.CompilerParams(
                collective_id=0, has_side_effects=True, vmem_limit_bytes=60 * 1024 * 1024
            ),
        )(
            *(
                pltpu.with_memory_space_constraint(a, pltpu.HBM)
                for a in (hidden.transpose(1, 0, 2), draft_ids.T, norm_gain.reshape(dim // LANES, LANES), head_w.T)
            )
        )
        logp, log_norm, entropy = pl.pallas_call(
            store_kernel,
            out_shape=tuple(jax.ShapeDtypeStruct(r.shape, r.dtype) for r in results),
            in_specs=[vmem] * len(results),
            out_specs=(pl.BlockSpec(memory_space=pl.ANY),) * len(results),
            scratch_shapes=[pltpu.SemaphoreType.DMA((len(results),))],
        )(*(pltpu.with_memory_space_constraint(r, pltpu.VMEM) for r in results))
        return logp.T, log_norm.T, entropy.T

    specs_in = (P('dp', None, None), P('dp', None), P(None), P(None, 'tp'))
    specs_out = (P('dp', None), P('dp', None), P('dp', None))
    return jax.shard_map(per_device, mesh=mesh, in_specs=specs_in, out_specs=specs_out, check_vma=False)
```

```python
import functools

import jax
import jax.numpy as jnp
from jax import lax
from jax.experimental import pallas as pl
from jax.experimental.pallas import tpu as pltpu
from jax.sharding import PartitionSpec as P

NORM_EPS = 1e-5
LANES = 128
SUBLANES = 8
PACKED = 16
CFG = {'sizes': (160, 256, 272, 272, 272, 272, 272, 224)}


def bounds_of(total, sizes):
    out, start = [], 0
    for size in sizes:
        size = min(size, total - start)
        if size:
            out.append((start, size))
        start += size
    out.extend((begin, min(sizes[-1], total - begin)) for begin in range(start, total, sizes[-1]))
    return out


def stats_of(carry, local_ids, start, tiles):
    top, exp_sum, weighted, picked = carry
    size, lanes = tiles.shape
    tiles = tiles.reshape(size // SUBLANES, SUBLANES, lanes)
    col_ids = lax.broadcasted_iota(jnp.int32, tiles.shape, 0) * SUBLANES + (
        lax.broadcasted_iota(jnp.int32, tiles.shape, 1) + start
    )
    hit = jnp.sum(jnp.where(col_ids == local_ids[None, :, :lanes], tiles, 0.0), axis=0)
    chunk_top = jnp.max(tiles, axis=0)
    new_top = chunk_top if top is None else jnp.maximum(top, chunk_top)
    shifted = tiles - new_top[None]
    exp_vals = jnp.exp(shifted)
    chunk_sum = jnp.sum(exp_vals, axis=0)
    chunk_weighted = jnp.sum(exp_vals * shifted, axis=0)
    if top is None:
        return new_top, chunk_sum, chunk_weighted, hit
    drop = top - new_top
    scale = jnp.exp(drop)
    return (
        new_top,
        chunk_sum + scale * exp_sum,
        chunk_weighted + scale * (weighted + exp_sum * drop),
        picked + hit,
    )


def fold(carry, rows, drafts):
    top, exp_sum, weighted, picked = carry
    all_top = jnp.max(top, axis=0, keepdims=True)
    drop = top - all_top
    scale = jnp.exp(drop)
    out = [
        all_top,
        jnp.sum(scale * exp_sum, axis=0, keepdims=True),
        jnp.sum(scale * (weighted + exp_sum * drop), axis=0, keepdims=True),
    ]
    picked = jnp.sum(picked, axis=0, keepdims=True)
    spare = LANES - rows
    for t in range(len(out)):
        lanes = picked[:, t * spare:(t + 1) * spare] if t < drafts else jnp.zeros((1, spare), jnp.float32)
        out[t] = jnp.concatenate([out[t], lanes], axis=1)
    return jnp.concatenate(out, axis=0)


def local_scratch(steps, seqs, drafts, dim, cols, pieces):
    return [
        pltpu.VMEM((steps, seqs, dim), jnp.bfloat16),
        pltpu.VMEM((drafts, seqs), jnp.int32),
        pltpu.VMEM((dim // LANES, LANES), jnp.bfloat16),
        pltpu.VMEM((dim // LANES, LANES), jnp.float32),
        pltpu.VMEM((steps * seqs, dim), jnp.bfloat16),
        pltpu.VMEM((cols, dim), jnp.bfloat16),
        pltpu.SemaphoreType.DMA((steps,)),
        pltpu.SemaphoreType.DMA((2,)),
        pltpu.SemaphoreType.DMA((pieces,)),
    ]


def local_stats(cfg, me, x_hbm, ids_hbm, gain_hbm, w_hbm, x_vmem, ids_vmem, gain_vmem, gain_wide, n_vmem, w_vmem,
                x_sem, small_sem, w_sem, announce):
    steps, seqs, dim = x_vmem.shape
    drafts = ids_vmem.shape[0]
    cols = w_vmem.shape[0]
    chunks = bounds_of(cols, cfg['sizes'])

    gain_copy = pltpu.make_async_copy(gain_hbm, gain_vmem, small_sem.at[1])
    ids_copy = pltpu.make_async_copy(ids_hbm, ids_vmem, small_sem.at[0])
    x_copies = [pltpu.make_async_copy(x_hbm.at[t], x_vmem.at[t], x_sem.at[t]) for t in range(steps)]
    depths = (pl.ds(0, dim // 2), pl.ds(dim // 2, dim // 2))
    w_copies = []
    for i, (start, size) in enumerate(chunks):
        for depth in depths:
            where = (pl.ds(start, size), depth)
            w_copies.append(pltpu.make_async_copy(w_hbm.at[where], w_vmem.at[where], w_sem.at[len(w_copies)]))
    for copy in [gain_copy, ids_copy] + x_copies:
        copy.start()
    announce(0, 1)
    for copy in w_copies:
        copy.start()
    announce(1, None)

    groups = [(t, g) for t in range(steps) for g in range(0, seqs, PACKED)]

    def block(t, g, c):
        return x_vmem[t, pl.ds(g, PACKED), pl.ds(c * LANES, LANES)].astype(jnp.float32)

    ids_copy.wait()
    ids = jnp.concatenate(
        [ids_vmem[pl.ds(t, 1), :] for t in range(drafts)] + [jnp.full((1, LANES - drafts * seqs), -1, jnp.int32)],
        axis=1,
    )
    local_ids = ids - me * cols
    gain_copy.wait()
    gain_wide[...] = gain_vmem[...].astype(jnp.float32)
    squares = {}
    for t in range(steps):
        x_copies[t].wait()
        for tt, g in groups:
            if tt == t:
                sums = [None] * 4
                for c in range(dim // LANES):
                    x = block(t, g, c)
                    sums[c % 4] = x * x if sums[c % 4] is None else sums[c % 4] + x * x
                squares[t, g] = (sums[0] + sums[1]) + (sums[2] + sums[3])
    inv_rms = {}
    for key in groups:
        inv_rms[key] = lax.rsqrt(jnp.sum(squares[key], axis=-1, keepdims=True) / dim + NORM_EPS)
    for t, g in groups:
        for c in range(dim // LANES):
            n = block(t, g, c) * inv_rms[t, g] * gain_wide[pl.ds(c, 1), :]
            n_vmem[pl.ds(t * seqs + g, PACKED), pl.ds(c * LANES, LANES)] = n.astype(jnp.bfloat16)

    def product(begin, part, depth):
        return lax.dot_general(
            w_vmem[pl.ds(begin, part), depth], n_vmem[:, depth], (((1,), (1,)), ((), ())),
            preferred_element_type=jnp.float32,
        )

    carry = (None,) * 4
    opened = []
    for i in range(len(chunks) + 1):
        if i:
            w_copies[2 * i - 1].wait()
        if i < len(chunks):
            w_copies[2 * i].wait()
        closed = [(begin, part, tiles + product(begin, part, depths[1])) for begin, part, tiles in opened]
        opened = []
        if i < len(chunks):
            start, size = chunks[i]
            first = -(-size // 2 // PACKED) * PACKED
            for begin, part in ((start, first), (start + first, size - first)):
                low, high = (product(begin, part, pl.ds(j * (dim // 4), dim // 4)) for j in range(2))
                opened.append((begin, part, low + high))
        for begin, _, tiles in closed:
            carry = stats_of(carry, local_ids, begin, tiles)
    return fold(carry, steps * seqs, drafts)


def head_kernel(
    cfg, peers,
    x_hbm, ids_hbm, gain_hbm, w_hbm,
    logp_ref, norm_ref, ent_ref,
    own, recv, sent, send_sem, recv_sem, *scratch,
):
    steps, seqs, _ = scratch[0].shape
    drafts = scratch[1].shape[0]
    me = lax.axis_index('tp')
    targets = [other + jnp.where(other >= me, 1, 0) for other in range(peers - 1)]
    barrier = pltpu.get_barrier_semaphore()

    def announce(begin, end):
        for target in targets[begin:end]:
            pl.semaphore_signal(barrier, inc=1, device_id={'tp': target}, device_id_type=pl.DeviceIdType.MESH)

    stats = local_stats(cfg, me, x_hbm, ids_hbm, gain_hbm, w_hbm, *scratch, announce)
    own[...] = stats
    slot = pl.ds(pl.multiple_of(me * SUBLANES, SUBLANES), stats.shape[0])
    recv[slot, :] = stats

    pl.semaphore_wait(barrier, peers - 1)
    for target in targets:
        pltpu.make_async_remote_copy(
            src_ref=own, dst_ref=recv.at[slot], send_sem=send_sem, recv_sem=recv_sem,
            device_id={'tp': target}, device_id_type=pl.DeviceIdType.MESH,
        ).start()
    others = sent.at[pl.ds(0, peers - 1)]
    pltpu.make_async_copy(others, others, recv_sem).wait()

    tops, sums, weights = parts = [recv[pl.ds(i, peers, stride=SUBLANES), :] for i in range(3)]
    rows = steps * seqs
    lane = lax.broadcasted_iota(jnp.int32, (1, LANES), 1)
    picked = jnp.zeros((1, LANES), jnp.float32)
    for t in range(drafts):
        turned = pltpu.roll(jnp.sum(parts[t], axis=0, keepdims=True), (t * seqs - rows) % LANES, 1)
        picked = jnp.where((lane >= t * seqs) & (lane < (t + 1) * seqs), turned, picked)
    full_top = jnp.max(tops, axis=0, keepdims=True)
    drop = tops - full_top
    scale = jnp.exp(drop)
    full_sum = jnp.sum(scale * sums, axis=0, keepdims=True)
    full_weighted = jnp.sum(scale * (weights + sums * drop), axis=0, keepdims=True)
    log_sum = jnp.log(full_sum)
    entropy = log_sum - full_weighted / full_sum

    log_norm = full_top + log_sum
    logp = picked - log_norm
    for t in range(steps):
        lanes = slice(t * seqs, (t + 1) * seqs)
        norm_ref[pl.ds(t, 1), :] = log_norm[:, lanes]
        ent_ref[pl.ds(t, 1), :] = entropy[:, lanes]
        if t < drafts:
            logp_ref[pl.ds(t, 1), :] = logp[:, lanes]
    pltpu.make_async_copy(others, others, send_sem).wait()


def store_kernel(*refs):
    count = (len(refs) - 1) // 2
    copies = [pltpu.make_async_copy(refs[i], refs[count + i], refs[-1].at[i]) for i in range(count)]
    for copy in copies:
        copy.start()
    for copy in copies:
        copy.wait()


def solution(mesh):
    peers = mesh.shape['tp']

    def per_device(hidden, draft_ids, norm_gain, head_w):
        seqs, steps, dim = hidden.shape
        drafts = draft_ids.shape[1]
        cols = head_w.shape[1]
        assert steps >= drafts and seqs == LANES - steps * seqs
        vmem = pl.BlockSpec(memory_space=pltpu.VMEM)
        results = pl.pallas_call(
            functools.partial(head_kernel, CFG, peers),
            out_shape=tuple(pltpu.VMEM((n, seqs), jnp.float32) for n in (drafts, steps, steps)),
            in_specs=[pl.BlockSpec(memory_space=pltpu.HBM)] * 4,
            out_specs=(vmem,) * 3,
            scratch_shapes=[
                pltpu.VMEM((3, LANES), jnp.float32),
                pltpu.VMEM((peers * SUBLANES, LANES), jnp.float32),
                pltpu.VMEM((peers, 3, LANES), jnp.float32),
                pltpu.SemaphoreType.DMA,
                pltpu.SemaphoreType.DMA,
            ] + local_scratch(steps, seqs, drafts, dim, cols, 2 * len(bounds_of(cols, CFG['sizes']))),
            compiler_params=pltpu.CompilerParams(
                collective_id=0, has_side_effects=True, vmem_limit_bytes=60 * 1024 * 1024
            ),
        )(
            *(
                pltpu.with_memory_space_constraint(a, pltpu.HBM)
                for a in (hidden.transpose(1, 0, 2), draft_ids.T, norm_gain.reshape(dim // LANES, LANES), head_w.T)
            )
        )
        logp, log_norm, entropy = pl.pallas_call(
            store_kernel,
            out_shape=tuple(jax.ShapeDtypeStruct(r.shape, r.dtype) for r in results),
            in_specs=[vmem] * len(results),
            out_specs=(pl.BlockSpec(memory_space=pl.ANY),) * len(results),
            scratch_shapes=[pltpu.SemaphoreType.DMA((len(results),))],
        )(*(pltpu.with_memory_space_constraint(r, pltpu.VMEM) for r in results))
        return logp.T, log_norm.T, entropy.T

    specs_in = (P('dp', None, None), P('dp', None), P(None), P(None, 'tp'))
    specs_out = (P('dp', None), P('dp', None), P('dp', None))
    return jax.shard_map(per_device, mesh=mesh, in_specs=specs_in, out_specs=specs_out, check_vma=False)
```

```python
import functools

import jax
import jax.numpy as jnp
from jax import lax
from jax.experimental import pallas as pl
from jax.experimental.pallas import tpu as pltpu
from jax.sharding import PartitionSpec as P

NORM_EPS = 1e-5
LANES = 128
SUBLANES = 8
PACKED = 16
CFG = {'sizes': (160, 240, 256, 272, 272, 272, 272, 256)}


def bounds_of(total, sizes):
    out, start = [], 0
    for size in sizes:
        size = min(size, total - start)
        if size:
            out.append((start, size))
        start += size
    out.extend((begin, min(sizes[-1], total - begin)) for begin in range(start, total, sizes[-1]))
    return out


def stats_of(carry, local_ids, start, tiles):
    top, exp_sum, weighted, picked = carry
    size, lanes = tiles.shape
    tiles = tiles.reshape(size // SUBLANES, SUBLANES, lanes)
    col_ids = lax.broadcasted_iota(jnp.int32, tiles.shape, 0) * SUBLANES + (
        lax.broadcasted_iota(jnp.int32, tiles.shape, 1) + start
    )
    hit = jnp.sum(jnp.where(col_ids == local_ids[None, :, :lanes], tiles, 0.0), axis=0)
    chunk_top = jnp.max(tiles, axis=0)
    new_top = chunk_top if top is None else jnp.maximum(top, chunk_top)
    shifted = tiles - new_top[None]
    exp_vals = jnp.exp(shifted)
    chunk_sum = jnp.sum(exp_vals, axis=0)
    chunk_weighted = jnp.sum(exp_vals * shifted, axis=0)
    if top is None:
        return new_top, chunk_sum, chunk_weighted, hit
    drop = top - new_top
    scale = jnp.exp(drop)
    return (
        new_top,
        chunk_sum + scale * exp_sum,
        chunk_weighted + scale * (weighted + exp_sum * drop),
        picked + hit,
    )


def fold(carry, rows, drafts):
    top, exp_sum, weighted, picked = carry
    all_top = jnp.max(top, axis=0, keepdims=True)
    drop = top - all_top
    scale = jnp.exp(drop)
    out = [
        all_top,
        jnp.sum(scale * exp_sum, axis=0, keepdims=True),
        jnp.sum(scale * (weighted + exp_sum * drop), axis=0, keepdims=True),
    ]
    picked = jnp.sum(picked, axis=0, keepdims=True)
    spare = LANES - rows
    for t in range(len(out)):
        lanes = picked[:, t * spare:(t + 1) * spare] if t < drafts else jnp.zeros((1, spare), jnp.float32)
        out[t] = jnp.concatenate([out[t], lanes], axis=1)
    return jnp.concatenate(out, axis=0)


def local_scratch(steps, seqs, drafts, dim, cols, pieces):
    return [
        pltpu.VMEM((steps, seqs, dim), jnp.bfloat16),
        pltpu.VMEM((drafts, seqs), jnp.int32),
        pltpu.VMEM((dim // LANES, LANES), jnp.bfloat16),
        pltpu.VMEM((dim // LANES, LANES), jnp.float32),
        pltpu.VMEM((steps * seqs, dim), jnp.bfloat16),
        pltpu.VMEM((cols, dim), jnp.bfloat16),
        pltpu.SemaphoreType.DMA((steps,)),
        pltpu.SemaphoreType.DMA((2,)),
        pltpu.SemaphoreType.DMA((pieces,)),
    ]


def local_stats(cfg, me, x_hbm, ids_hbm, gain_hbm, w_hbm, x_vmem, ids_vmem, gain_vmem, gain_wide, n_vmem, w_vmem,
                x_sem, small_sem, w_sem, announce):
    steps, seqs, dim = x_vmem.shape
    drafts = ids_vmem.shape[0]
    cols = w_vmem.shape[0]
    chunks = bounds_of(cols, cfg['sizes'])

    gain_copy = pltpu.make_async_copy(gain_hbm, gain_vmem, small_sem.at[1])
    ids_copy = pltpu.make_async_copy(ids_hbm, ids_vmem, small_sem.at[0])
    x_copies = [pltpu.make_async_copy(x_hbm.at[t], x_vmem.at[t], x_sem.at[t]) for t in range(steps)]
    depths = (pl.ds(0, dim // 2), pl.ds(dim // 2, dim // 2))
    w_copies = []
    for i, (start, size) in enumerate(chunks):
        for depth in depths:
            where = (pl.ds(start, size), depth)
            w_copies.append(pltpu.make_async_copy(w_hbm.at[where], w_vmem.at[where], w_sem.at[len(w_copies)]))
    for copy in [gain_copy, ids_copy] + x_copies:
        copy.start()
    announce(0, 1)
    for copy in w_copies:
        copy.start()
    announce(1, None)

    groups = [(t, g) for t in range(steps) for g in range(0, seqs, PACKED)]

    def block(t, g, c):
        return x_vmem[t, pl.ds(g, PACKED), pl.ds(c * LANES, LANES)].astype(jnp.float32)

    ids_copy.wait()
    ids = jnp.concatenate(
        [ids_vmem[pl.ds(t, 1), :] for t in range(drafts)] + [jnp.full((1, LANES - drafts * seqs), -1, jnp.int32)],
        axis=1,
    )
    local_ids = ids - me * cols
    gain_copy.wait()
    gain_wide[...] = gain_vmem[...].astype(jnp.float32)
    squares = {}
    for t in range(steps):
        x_copies[t].wait()
        for tt, g in groups:
            if tt == t:
                sums = [None] * 4
                for c in range(dim // LANES):
                    x = block(t, g, c)
                    sums[c % 4] = x * x if sums[c % 4] is None else sums[c % 4] + x * x
                squares[t, g] = (sums[0] + sums[1]) + (sums[2] + sums[3])
    inv_rms = {}
    for key in groups:
        inv_rms[key] = lax.rsqrt(jnp.sum(squares[key], axis=-1, keepdims=True) / dim + NORM_EPS)
    for t, g in groups:
        for c in range(dim // LANES):
            n = block(t, g, c) * inv_rms[t, g] * gain_wide[pl.ds(c, 1), :]
            n_vmem[pl.ds(t * seqs + g, PACKED), pl.ds(c * LANES, LANES)] = n.astype(jnp.bfloat16)

    def product(begin, part, depth):
        return lax.dot_general(
            w_vmem[pl.ds(begin, part), depth], n_vmem[:, depth], (((1,), (1,)), ((), ())),
            preferred_element_type=jnp.float32,
        )

    carry = (None,) * 4
    opened = []
    for i in range(len(chunks) + 1):
        if i:
            w_copies[2 * i - 1].wait()
        if i < len(chunks):
            w_copies[2 * i].wait()
        closed = [(begin, part, tiles + product(begin, part, depths[1])) for begin, part, tiles in opened]
        opened = []
        if i < len(chunks):
            start, size = chunks[i]
            first = -(-size // 2 // PACKED) * PACKED
            for begin, part in ((start, first), (start + first, size - first)):
                low, high = (product(begin, part, pl.ds(j * (dim // 4), dim // 4)) for j in range(2))
                opened.append((begin, part, low + high))
        for begin, _, tiles in closed:
            carry = stats_of(carry, local_ids, begin, tiles)
    return fold(carry, steps * seqs, drafts)


def head_kernel(
    cfg, peers,
    x_hbm, ids_hbm, gain_hbm, w_hbm,
    logp_ref, norm_ref, ent_ref,
    own, recv, sent, send_sem, recv_sem, *scratch,
):
    steps, seqs, _ = scratch[0].shape
    drafts = scratch[1].shape[0]
    me = lax.axis_index('tp')
    targets = [other + jnp.where(other >= me, 1, 0) for other in range(peers - 1)]
    barrier = pltpu.get_barrier_semaphore()

    def announce(begin, end):
        for target in targets[begin:end]:
            pl.semaphore_signal(barrier, inc=1, device_id={'tp': target}, device_id_type=pl.DeviceIdType.MESH)

    stats = local_stats(cfg, me, x_hbm, ids_hbm, gain_hbm, w_hbm, *scratch, announce)
    own[...] = stats
    slot = pl.ds(pl.multiple_of(me * SUBLANES, SUBLANES), stats.shape[0])
    recv[slot, :] = stats

    pl.semaphore_wait(barrier, peers - 1)
    for target in targets:
        pltpu.make_async_remote_copy(
            src_ref=own, dst_ref=recv.at[slot], send_sem=send_sem, recv_sem=recv_sem,
            device_id={'tp': target}, device_id_type=pl.DeviceIdType.MESH,
        ).start()
    others = sent.at[pl.ds(0, peers - 1)]
    pltpu.make_async_copy(others, others, recv_sem).wait()

    tops, sums, weights = parts = [recv[pl.ds(i, peers, stride=SUBLANES), :] for i in range(3)]
    rows = steps * seqs
    lane = lax.broadcasted_iota(jnp.int32, (1, LANES), 1)
    picked = jnp.zeros((1, LANES), jnp.float32)
    for t in range(drafts):
        turned = pltpu.roll(jnp.sum(parts[t], axis=0, keepdims=True), (t * seqs - rows) % LANES, 1)
        picked = jnp.where((lane >= t * seqs) & (lane < (t + 1) * seqs), turned, picked)
    full_top = jnp.max(tops, axis=0, keepdims=True)
    drop = tops - full_top
    scale = jnp.exp(drop)
    full_sum = jnp.sum(scale * sums, axis=0, keepdims=True)
    full_weighted = jnp.sum(scale * (weights + sums * drop), axis=0, keepdims=True)
    log_sum = jnp.log(full_sum)
    entropy = log_sum - full_weighted / full_sum

    log_norm = full_top + log_sum
    logp = picked - log_norm
    for t in range(steps):
        lanes = slice(t * seqs, (t + 1) * seqs)
        norm_ref[pl.ds(t, 1), :] = log_norm[:, lanes]
        ent_ref[pl.ds(t, 1), :] = entropy[:, lanes]
        if t < drafts:
            logp_ref[pl.ds(t, 1), :] = logp[:, lanes]
    pltpu.make_async_copy(others, others, send_sem).wait()


def store_kernel(*refs):
    count = (len(refs) - 1) // 2
    copies = [pltpu.make_async_copy(refs[i], refs[count + i], refs[-1].at[i]) for i in range(count)]
    for copy in copies:
        copy.start()
    for copy in copies:
        copy.wait()


def solution(mesh):
    peers = mesh.shape['tp']

    def per_device(hidden, draft_ids, norm_gain, head_w):
        seqs, steps, dim = hidden.shape
        drafts = draft_ids.shape[1]
        cols = head_w.shape[1]
        assert steps >= drafts and seqs == LANES - steps * seqs
        vmem = pl.BlockSpec(memory_space=pltpu.VMEM)
        results = pl.pallas_call(
            functools.partial(head_kernel, CFG, peers),
            out_shape=tuple(pltpu.VMEM((n, seqs), jnp.float32) for n in (drafts, steps, steps)),
            in_specs=[pl.BlockSpec(memory_space=pltpu.HBM)] * 4,
            out_specs=(vmem,) * 3,
            scratch_shapes=[
                pltpu.VMEM((3, LANES), jnp.float32),
                pltpu.VMEM((peers * SUBLANES, LANES), jnp.float32),
                pltpu.VMEM((peers, 3, LANES), jnp.float32),
                pltpu.SemaphoreType.DMA,
                pltpu.SemaphoreType.DMA,
            ] + local_scratch(steps, seqs, drafts, dim, cols, 2 * len(bounds_of(cols, CFG['sizes']))),
            compiler_params=pltpu.CompilerParams(
                collective_id=0, has_side_effects=True, vmem_limit_bytes=60 * 1024 * 1024
            ),
        )(
            *(
                pltpu.with_memory_space_constraint(a, pltpu.HBM)
                for a in (hidden.transpose(1, 0, 2), draft_ids.T, norm_gain.reshape(dim // LANES, LANES), head_w.T)
            )
        )
        logp, log_norm, entropy = pl.pallas_call(
            store_kernel,
            out_shape=tuple(jax.ShapeDtypeStruct(r.shape, r.dtype) for r in results),
            in_specs=[vmem] * len(results),
            out_specs=(pl.BlockSpec(memory_space=pl.ANY),) * len(results),
            scratch_shapes=[pltpu.SemaphoreType.DMA((len(results),))],
        )(*(pltpu.with_memory_space_constraint(r, pltpu.VMEM) for r in results))
        return logp.T, log_norm.T, entropy.T

    specs_in = (P('dp', None, None), P('dp', None), P(None), P(None, 'tp'))
    specs_out = (P('dp', None), P('dp', None), P('dp', None))
    return jax.shard_map(per_device, mesh=mesh, in_specs=specs_in, out_specs=specs_out, check_vma=False)
```
